32 devices in a mesh: gx: 4 (over y, x), gy: 4 (over z), gz: 2 (over core).
Axes of the slice: x: 2, y: 2, z: 4, core: 2. Of those that a mesh axis runs over, the one named last changes fastest.
Arguments:
- start: float32 [4, 4, 2, 1, 32, 1024], P('gx', 'gy', 'gz'), may hold values from -6 to 6
- stencils: float32 [6, 4, 4, 2, 32, 32], P(None, 'gx', 'gy', 'gz'), as said below
Outputs:
- basis: float32 [4, 4, 2, 1, 5, 32, 1024], P('gx', 'gy', 'gz')
- coefficients: float32 [1, 2, 5], replicated
The draws below stay inside these ranges and needn't reach their ends.
Inputs may be any that keep to these rules, and one draw needn't show every extreme that they name: `stencils`: each of a patch's six matrices is symmetric positive definite.
All inputs are finite; a program needn't handle non-finite values.
Results may differ from the reference program's by a relative error of at most 0.0003.
Values sent between devices are 32-bit elements; how exact they have to be, the bound alone decides.
A program may use at most 128 MiB of HBM per device.

```python
import jax
import jax.numpy as jnp
from jax import lax

C = 32
PROBES = 1
ITERS = 5
PATCH_X = 4
PATCH_Y = 4
PATCH_Z = 2
N_GX = 4
N_GY = 4
N_GZ = 2


def draw_stencils(key, part):
    key_entries = jax.random.fold_in(key, 11)
    key_scale = jax.random.fold_in(key, 12)
    shape = (6, PATCH_X, PATCH_Y, PATCH_Z, C, C)
    entries = jax.random.normal(key_entries, shape, jnp.float32)
    rows = jnp.arange(C)
    band = (jnp.abs(rows[:, None] - rows[None, :]) <= 4).astype(jnp.float32)
    factor = entries * band
    square = jnp.einsum('...ij,...kj->...ik', factor, factor) / 9.0
    square = square + 0.5 * jnp.eye(C, dtype=jnp.float32)
    scales = jnp.exp(jax.random.uniform(key_scale, (6, PATCH_X, PATCH_Y, PATCH_Z, 1, 1), jnp.float32, -0.7, 0.7))
    return (square * scales).astype(jnp.float32)


def level_of(stream_key, shape, cuts, smallest, high):
    loudness = 1.0
    for axis_at, blocks in cuts:
        steps = jax.random.uniform(jax.random.fold_in(jax.random.fold_in(stream_key, 6), axis_at), (blocks,), jnp.float32, smallest / len(cuts), high / len(cuts))
        loudness = loudness * jnp.repeat(jnp.exp(steps), shape[axis_at] // blocks).reshape((-1,) + (1,) * (len(shape) - 1 - axis_at))
    return loudness


def bell_draw(rng, extent, spread, bound, pieces=(), held_as=jnp.bfloat16):
    result = jax.random.normal(rng, extent, jnp.float32) * spread
    if len(pieces) > 0:
        result = level_of(rng, extent, pieces, -0.22, 0.18) * result
    return jnp.clip(result, min=-bound, max=bound).astype(held_as)


def setup_inputs(seed: int = 0) -> dict:
    splits = jax.random.split(jax.random.key(seed), 3)
    return {
        "start": bell_draw(splits[0], (PATCH_X, PATCH_Y, PATCH_Z, PROBES, C, C * C), 1.0, 6.0, ((0, 4), (1, 4), (2, 2)), jnp.float32),
        "stencils": draw_stencils(jax.random.fold_in(splits[2], 71), 0),
    }


def along(field, stencils, which, dim):
    grid = field.reshape(N_GX, C, N_GY, C, N_GZ, C)
    matrix = stencils[which]
    forms = ['xaybzc,xyzea->xeybzc', 'xaybzc,xyzeb->xayezc', 'xaybzc,xyzec->xaybze']
    out = jnp.einsum(forms[dim], grid, matrix, precision=lax.Precision.HIGHEST)
    return out.reshape(N_GX * C, N_GY * C, N_GZ * C)

def fold(field, dim, groups):
    moved = jnp.moveaxis(field, dim, 0)
    rest = moved.shape[1:]
    blocks = moved.reshape((groups, C) + rest)
    zero_row = jnp.zeros((1,) + rest, jnp.float32)
    first = blocks[:, 0] + jnp.concatenate([zero_row, blocks[:-1, C - 1]], axis=0)
    last = blocks[:, C - 1] + jnp.concatenate([blocks[1:, 0], zero_row], axis=0)
    blocks = blocks.at[:, 0].set(first).at[:, C - 1].set(last)
    return jnp.moveaxis(blocks.reshape((groups * C,) + rest), 0, dim)

def assemble(field):
    field = fold(field, 0, N_GX)
    field = fold(field, 1, N_GY)
    return fold(field, 2, N_GZ)

def weight_vector(groups):
    index = jnp.arange(groups * C)
    plane = index % C
    block = index // C
    shared = (plane == 0) & (block > 0) | (plane == C - 1) & (block < groups - 1)
    return jnp.where(shared, 0.5, 1.0).astype(jnp.float32)

def operate(field, stencils):
    first = along(field, stencils, 5, 2)
    second = along(first, stencils, 4, 1)
    term_one = along(second, stencils, 0, 0)
    third = along(first, stencils, 1, 1)
    fourth = along(field, stencils, 2, 2)
    fifth = along(fourth, stencils, 4, 1)
    term_two = along(third + fifth, stencils, 3, 0)
    return assemble(term_one + term_two)

def single(start_one, stencils, weights):
    first = assemble(weights * start_one)
    vector = first / jnp.sqrt(jnp.sum(weights * first * first))
    vectors = [vector]
    alphas = []
    betas = []
    for j in range(ITERS):
        image = operate(vectors[j], stencils)
        alpha = jnp.sum(weights * image * vectors[j])
        image = image - alpha * vectors[j]
        if j > 0:
            image = image - betas[j - 1] * vectors[j - 1]
        heights = [jnp.sum(weights * basis_vec * image) for basis_vec in vectors]
        for i in range(j + 1):
            image = image - heights[i] * vectors[i]
        beta = jnp.sqrt(jnp.sum(weights * image * image))
        vectors.append(image / beta)
        alphas.append(alpha)
        betas.append(beta)
    coeffs = jnp.stack([jnp.stack(alphas), jnp.stack(betas)])
    return (jnp.stack(vectors[1:]), coeffs)

def reference(start, stencils):
    weights = weight_vector(N_GX)[:, None, None] * weight_vector(N_GY)[None, :, None] * weight_vector(N_GZ)[None, None, :]
    seven = start.reshape(N_GX, N_GY, N_GZ, PROBES, C, C, C)
    whole = jnp.transpose(seven, (3, 0, 4, 1, 5, 2, 6)).reshape(PROBES, N_GX * C, N_GY * C, N_GZ * C)
    basis_whole, coefficients = lax.map(lambda one: single(one, stencils, weights), whole)
    split = basis_whole.reshape(PROBES, ITERS, N_GX, C, N_GY, C, N_GZ, C)
    basis = jnp.transpose(split, (2, 4, 6, 0, 1, 3, 5, 7)).reshape(N_GX, N_GY, N_GZ, PROBES, ITERS, C, C * C)
    return (basis, coefficients)
```

```python
import functools

import jax
import jax.numpy as jnp
from jax import lax
from jax.experimental import pallas as pl
from jax.experimental.pallas import tpu as pltpu
from jax.sharding import PartitionSpec as P

ITERS = 5
LANES = 128
SUB = 8
MESH = pl.DeviceIdType.MESH
F32 = jnp.float32
BF16 = jnp.bfloat16
HIGHEST = lax.Precision.HIGHEST


def iota(shape, dim):
    return lax.broadcasted_iota(jnp.int32, shape, dim)


def split(x):
    hi = x.astype(BF16)
    return hi, (x - hi.astype(F32)).astype(BF16)


def exact(a, b):
    return lax.dot_general(a, b, (((1,), (0,)), ((), ())), precision=HIGHEST, preferred_element_type=F32)


def mul(a, b):
    return jnp.dot(a, b, preferred_element_type=F32)


def swap(x):
    sub = iota((1, SUB, LANES), 1)
    group = iota((1, SUB, LANES), 2) >> 5
    s0, s1 = sub & 1, (sub >> 1) & 1
    g0, g1 = group & 1, (group >> 1) & 1
    far = pltpu.roll(x, 64, 2)
    x = jnp.where(s1 == g1, x, jnp.where(s1 == 0, pltpu.roll(far, SUB - 2, 1), pltpu.roll(far, 2, 1)))
    up = pltpu.roll(pltpu.roll(x, SUB - 1, 1), 32, 2)
    down = pltpu.roll(pltpu.roll(x, 1, 1), LANES - 32, 2)
    return jnp.where(s0 == g0, x, jnp.where(s0 == 0, up, down))


def build_matrices(st, mx, my, mz):
    count = st.shape[1]
    wide = LANES
    spread = ((iota((wide, count), 0) & (count - 1)) == iota((wide, count), 1)).astype(F32)
    spread_t = ((iota((count, wide), 1) & (count - 1)) == iota((count, wide), 0)).astype(F32)
    same = (iota((wide, wide), 0) >> 5) == (iota((wide, wide), 1) >> 5)
    for slot, which in ((0, 5), (1, 2)):
        big = exact(exact(spread, st[which].T), spread_t)
        hi, lo = split(jnp.where(same, big, 0.0))
        mz[0:wide, slot * wide:(slot + 1) * wide] = hi
        mz[wide:2 * wide, slot * wide:(slot + 1) * wide] = hi
        mz[2 * wide:3 * wide, slot * wide:(slot + 1) * wide] = lo
    rows = 2 * count
    r = iota((rows, count), 0)
    pick = (((r >> 3) * 4 + (r & 3)) == iota((rows, count), 1)).astype(F32)
    cols = 3 * rows
    l = iota((count, cols), 1) & (rows - 1)
    pick_t = (((l >> 3) * 4 + (l & 3)) == iota((count, cols), 0)).astype(F32)
    same = ((iota((rows, cols), 0) >> 2) & 1) == ((iota((rows, cols), 1) >> 2) & 1)
    middle = (iota((rows, cols), 1) >= rows) & (iota((rows, cols), 1) < 2 * rows)
    for slot, which in ((0, 4), (1, 1)):
        big = jnp.where(same, exact(exact(pick, st[which]), pick_t), 0.0)
        hi = big.astype(BF16).astype(F32)
        my[slot * rows:(slot + 1) * rows, :] = jnp.where(middle, big - hi, hi).astype(BF16)
    cols = 6 * count
    tile = ((iota((count, cols), 1) & (count - 1)) == iota((count, cols), 0)).astype(F32)
    stiff = exact(st[0], tile)
    mass = exact(st[3], tile)
    block = iota((count, cols), 1) >> 5
    big = jnp.where(block < 3, stiff, mass)
    hi = big.astype(BF16).astype(F32)
    mx[...] = jnp.where((block == 1) | (block == 4), big - hi, hi).astype(BF16)


def apply_patch(u, mx, my, mz):
    count, area = u.shape
    ni, nt = count // SUB, area // LANES
    tiles = jnp.concatenate(
        [u[SUB * i:SUB * (i + 1), LANES * t:LANES * (t + 1)] for i in range(ni) for t in range(nt)], axis=0
    )
    tiles = swap(tiles.reshape(ni * nt, SUB, LANES)).reshape(ni * nt * SUB, LANES)
    hi, lo = split(tiles)
    z = mul(jnp.concatenate([hi, lo, hi], axis=1), mz)
    rows = nt * SUB
    packed = []
    for slot in range(2):
        part = z[:, slot * LANES:(slot + 1) * LANES]
        wide = jnp.concatenate([part[rows * i:rows * (i + 1)] for i in range(ni)], axis=1)
        hi, lo = split(wide)
        packed.append(jnp.concatenate([hi, hi, lo], axis=0))
    both = mul(my, packed[0])
    first = both[:rows]
    second = both[rows:] + mul(my[:rows], packed[1])
    pieces = []
    for term in (first, second):
        stacked = jnp.concatenate([term[:, LANES * i:LANES * (i + 1)] for i in range(ni)], axis=0)
        stacked = swap(stacked.reshape(ni * nt, SUB, LANES))
        back = jnp.concatenate(
            [jnp.concatenate([stacked[i * nt + t] for i in range(ni)], axis=0) for t in range(nt)], axis=1
        )
        hi, lo = split(back)
        pieces += [hi, hi, lo]
    return mul(mx, jnp.concatenate(pieces, axis=0))


def kernel(sizes, start_in, st_in, basis, coef, mx, my, mz, wt, v0, field,
           zs, zr, xs, xr, ys, yr, es, er, rows, hsend, hrecv, rsend, rrecv, ready, locals_, images, start, st, loads):
    load_start = pltpu.make_async_copy(start_in, start, loads.at[0])
    load_st = pltpu.make_async_copy(st_in, st, loads.at[1])
    load_start.start()
    load_st.start()
    nx, ny, nz = sizes
    total = nx * ny * nz
    count, area = start.shape
    nt = area // LANES
    ni = count // SUB
    last = count - 1
    px, py, pz = lax.axis_index("gx"), lax.axis_index("gy"), lax.axis_index("gz")
    me = (px * ny + py) * nz + pz
    coords = (px, py, pz)
    there = [[coords[d] > 0, coords[d] < sizes[d] - 1] for d in range(3)]

    for ref in (zr, xr, yr, er):
        ref[...] = jnp.zeros_like(ref)
    barrier = pltpu.get_barrier_semaphore()

    def peer(k):
        p = lax.rem(me + k, total)
        return (p // (ny * nz), (p // nz) % ny, p % nz)

    def every_peer(act):
        if total > 64:
            def step(k, carry):
                act(peer(k))
                return carry

            lax.fori_loop(1, total, step, 0)
            return
        around = [[lax.rem(coords[d] + k, sizes[d]) if k else coords[d] for k in range(sizes[d])] for d in range(3)]
        for ky in range(ny - 1, -1, -1):
            for kx in range(nx - 1, -1, -1):
                for kz in range(nz):
                    if kx or ky or kz:
                        act((around[0][kx], around[1][ky], around[2][kz]))

    def neighbours(act):
        for dx in (-1, 0, 1):
            for dy in (-1, 0, 1):
                for dz in (-1, 0, 1):
                    if dx or dy or dz:
                        target = (px + dx, py + dy, pz + dz)
                        inside = None
                        for d, step in enumerate((dx, dy, dz)):
                            if step:
                                side = there[d][(step + 1) // 2]
                                inside = side if inside is None else inside & side

                        @pl.when(inside)
                        def _():
                            act(target)

    around_me = 1
    for d in range(3):
        around_me = around_me * (1 + (coords[d] > 0).astype(jnp.int32) + (coords[d] < sizes[d] - 1).astype(jnp.int32))
    around_me = around_me - 1

    rounds = max(sizes) - 2

    def call(r):
        neighbours(lambda target: pl.semaphore_signal(ready.at[r], inc=1, device_id=target, device_id_type=MESH))

    neighbours(lambda target: pl.semaphore_signal(barrier, inc=1, device_id=target, device_id_type=MESH))

    def shared(index, d):
        return ((index == 0) & there[d][0]) | ((index == last) & there[d][1])

    lane = iota((count, area), 1)
    ia, ib, ic = iota((count, area), 0), lane >> 5, lane & (count - 1)
    half = lambda index, d: jnp.where(shared(index, d), 0.5, 1.0)
    weight = half(ia, 0) * half(ib, 1) * half(ic, 2)
    wt[...] = weight.astype(F32)
    load_start.wait()
    field[...] = start[...] * wt[...]

    lane_c = iota((count, LANES), 1)
    face_c = (lane_c & (count - 1) == 0) | (lane_c & (count - 1) == last)
    even = (lane_c & 1) == 0
    lane8 = iota((SUB, LANES), 1)
    low8, high8 = lane8 < count, lane8 >= LANES - count
    lane1 = iota((1, LANES), 1)
    diag = iota((SUB, LANES), 0) == lane8

    def tile(t):
        return slice(t * LANES, (t + 1) * LANES)

    def halo_copies(phase):
        out = []

        def add(src, dst, slot, *direction):
            there_all, target = None, {}
            for d, step in enumerate(direction):
                if step is not None:
                    there_all = there[d][step] if there_all is None else there_all & there[d][step]
            target = tuple(c if step is None else c + 2 * step - 1 for c, step in zip(coords, direction))
            copy = pltpu.make_async_remote_copy(
                src_ref=src, dst_ref=dst.at[phase, slot], send_sem=hsend.at[phase, len(out)],
                recv_sem=hrecv.at[phase, len(out)], device_id=target, device_id_type=MESH)
            out.append((copy, there_all, direction, dst, slot))

        for z in (1, 0, None):
            for d in range(2):
                for e in range(2):
                    back = 0 if z is None else 2 - z
                    add(es.at[phase, 2 * d + e], er, (2 * (1 - d) + 1 - e) * 3 + back, d, e, z)
        for z in (1, 0, None):
            back = 0 if z is None else 2 - z
            for d in range(2):
                add(xs.at[phase, d], xr, (1 - d) * 3 + back, d, None, z)
        for z in (1, 0, None):
            back = 0 if z is None else 2 - z
            for d in range(2):
                add(ys.at[phase, d], yr, (1 - d) * 3 + back, None, d, z)
        for d in range(2):
            add(zs.at[phase], zr, 1 - d, None, None, d)
        return out

    def start_all(copies):
        for copy, exists, *_ in copies:
            @pl.when(exists)
            def _():
                copy.start()

    def send_halo(phase):
        copies = halo_copies(phase)
        for d in range(2):
            row = 0 if d == 0 else last
            for e in range(2):
                es[phase, 2 * d + e] = field[row:row + 1, tile(0 if e == 0 else nt - 1)]
            for t in range(nt):
                xs[phase, d, t:t + 1, :] = field[row:row + 1, tile(t)]
            packed = None
            for i in range(ni):
                block = field[SUB * i:SUB * (i + 1), tile(0 if d == 0 else nt - 1)]
                part = jnp.where(low8 if d == 0 else high8, block, 0.0)
                shift = (count * i + d * count) % LANES
                part = part if shift == 0 else pltpu.roll(part, shift, 1)
                packed = part if packed is None else packed + part
            ys[phase, d] = packed
        packed = None
        for t in range(nt):
            part = jnp.where(face_c, field[:, tile(t)], 0.0)
            part = part if t == 0 else pltpu.roll(part, 2 * t, 1)
            packed = part if packed is None else packed + part
        zs[phase] = packed
        start_all(copies)

    def fold(ref, phase, base):
        low = ref[phase, base + 1]
        c = iota(low.shape, 1) & (count - 1)
        out = ref[phase, base] + jnp.where(c == 0, pltpu.roll(low, LANES - last, 1), 0.0)
        return out + jnp.where(c == last, pltpu.roll(ref[phase, base + 2], last, 1), 0.0)

    def add_halo(phase):
        copies = halo_copies(phase)
        for index, (copy, _, direction, dst, slot) in enumerate(copies):
            mirror = None
            for d, step in enumerate(direction):
                if step is not None:
                    mirror = there[d][1 - step] if mirror is None else mirror & there[d][1 - step]

            @pl.when(mirror)
            def _():
                into = dst.at[phase, slot]
                pltpu.make_async_copy(into, into, hrecv.at[phase, index]).wait()
        merged = jnp.where(even, pltpu.roll(zr[phase, 0], LANES - last, 1), pltpu.roll(zr[phase, 1], last, 1))
        for t in range(nt):
            part = merged if t == 0 else pltpu.roll(merged, LANES - 2 * t, 1)
            field[:, tile(t)] += jnp.where(face_c, part, 0.0)
        for d in range(2):
            received = fold(yr, phase, 3 * d)
            for i in range(ni):
                shift = (-count * i - d * count) % LANES
                part = received if shift == 0 else pltpu.roll(received, shift, 1)
                field[SUB * i:SUB * (i + 1), tile(0 if d == 0 else nt - 1)] += jnp.where(low8 if d == 0 else high8, part, 0.0)
        for d in range(2):
            row = 0 if d == 0 else last
            received = fold(xr, phase, 3 * d)
            for t in range(nt):
                line = received[t:t + 1]
                if t == 0:
                    line += jnp.where(lane1 < count, pltpu.roll(fold(er, phase, 6 * d), count, 1), 0.0)
                if t == nt - 1:
                    line += jnp.where(lane1 >= LANES - count, pltpu.roll(fold(er, phase, 6 * d + 3), LANES - count, 1), 0.0)
                field[row:row + 1, tile(t)] += line

    def send_dots(phase, products):
        packed = None
        for k, product in enumerate(products):
            acc = None
            for i in range(ni):
                for t in range(nt):
                    block = product[SUB * i:SUB * (i + 1), tile(t)]
                    acc = block if acc is None else acc + block
            line = jnp.where(iota((SUB, LANES), 0) == k, jnp.sum(acc, axis=0, keepdims=True), 0.0)
            packed = line if packed is None else packed + line
        sums = jnp.sum(packed, axis=1, keepdims=True)
        rows[phase, me] = jnp.sum(jnp.where(diag, sums, 0.0), axis=0, keepdims=True)

        def send(target):
            pltpu.make_async_remote_copy(
                src_ref=rows.at[phase, me], dst_ref=rows.at[phase, me], send_sem=rsend.at[phase],
                recv_sem=rrecv.at[phase], device_id=target, device_id_type=MESH).start()

        every_peer(send)

    def take_dots(phase):
        others = rows.at[phase, pl.ds(0, total - 1)]
        pltpu.make_async_copy(others, others, rrecv.at[phase]).wait()
        line = jnp.sum(rows[phase], axis=0)
        return jnp.sum(jnp.where(diag, line, 0.0), axis=1, keepdims=True)

    pl.semaphore_wait(barrier, around_me)
    send_halo(0)
    load_st.wait()
    build_matrices(st, mx, my, mz)
    for r in range(rounds):
        call(r)
        if r < rounds - 1:
            pl.semaphore_wait(ready.at[r], around_me)
    add_halo(0)
    vector = field[...]
    alpha = None
    row2, col2 = iota(coef.shape[1:], 0), iota(coef.shape[1:], 1)
    coefs = jnp.zeros(coef.shape[1:], F32)
    local = apply_patch(vector, mx[...], my[...], mz[...])
    field[...] = local
    send_halo(1)
    if rounds > 0:
        pl.semaphore_wait(ready.at[rounds - 1], around_me)
    send_dots(1, [wt[...] * vector * vector, local * vector])
    add_halo(1)
    image = field[...]
    for j in range(ITERS):
        more = j < ITERS - 1
        if more:
            ahead = apply_patch(image, mx[...], my[...], mz[...])
            field[...] = ahead
            send_halo(j + 2)
        sums = take_dots(j + 1)
        norm = jnp.sqrt(sums[0:1])
        inverse = 1.0 / norm
        if j > 0:
            coefs = jnp.where((row2 == 1) & (col2 == j - 1), norm * alpha, coefs)
        alpha = sums[1:2] / sums[0:1]
        coefs = jnp.where((row2 == 0) & (col2 == j), alpha, coefs)
        factor = inverse / alpha
        heights = [sums[2 + i:3 + i] * factor for i in range(j)]

        def follow(applied, unit, old):
            out = applied * factor - unit
            for i in range(j):
                out = out - heights[i] * old(i)
            return out

        old_vector = lambda i: v0[...] if i == 0 else basis[i - 1]
        unit = vector * inverse
        if j == 0:
            v0[...] = unit
        else:
            basis[j - 1] = unit
        vector = follow(image, unit, old_vector)
        if more:
            unit = local * inverse
            locals_[j] = unit
            local = follow(ahead, unit, lambda i: locals_[i])
            send_dots(j + 2, [wt[...] * vector * vector, local * vector] + [local * old_vector(i) for i in range(j + 1)])
            unit = image * inverse
            images[j] = unit
            add_halo(j + 2)
            image = follow(field[...], unit, lambda i: images[i])
    send_dots(ITERS + 1, [wt[...] * vector * vector])
    sums = take_dots(ITERS + 1)
    norm = jnp.sqrt(sums[0:1])
    coefs = jnp.where((row2 == 1) & (col2 == ITERS - 1), norm * alpha, coefs)
    basis[ITERS - 1] = vector * (1.0 / norm)
    coef[0] = coefs

    for phase in range(ITERS + 1):
        for copy, exists, *_ in halo_copies(phase):
            @pl.when(exists)
            def _():
                copy.wait_send()
    for phase in range(1, ITERS + 2):
        others = rows.at[phase, pl.ds(0, total - 1)]
        pltpu.make_async_copy(others, others, rsend.at[phase]).wait()


def store(basis, coef, basis_out, coef_out, sems):
    copies = [pltpu.make_async_copy(basis.at[i], basis_out.at[i], sems.at[i]) for i in range(ITERS)]
    copies.append(pltpu.make_async_copy(coef, coef_out, sems.at[ITERS]))
    for copy in copies:
        copy.start()
    for copy in copies:
        copy.wait()


def shards(sizes, start, stencils):
    probes, count, area = start.shape[3:]
    nt = area // LANES
    total = sizes[0] * sizes[1] * sizes[2]
    halos = ITERS + 1
    vmem = pl.BlockSpec(memory_space=pltpu.VMEM)
    call_shapes = (jax.ShapeDtypeStruct((ITERS, count, area), F32), jax.ShapeDtypeStruct((1, 2, ITERS), F32))
    call = pl.pallas_call(
        functools.partial(kernel, sizes),
        out_shape=call_shapes,
        in_specs=[pl.BlockSpec(memory_space=pltpu.HBM)] * 2,
        out_specs=(vmem, vmem),
        scratch_shapes=[
            pltpu.VMEM((count, 6 * count), BF16),
            pltpu.VMEM((4 * count, 6 * count), BF16),
            pltpu.VMEM((3 * LANES, 2 * LANES), BF16),
            pltpu.VMEM((count, area), F32),
            pltpu.VMEM((count, area), F32),
            pltpu.VMEM((count, area), F32),
            pltpu.VMEM((halos, count, LANES), F32),
            pltpu.VMEM((halos, 2, count, LANES), F32),
            pltpu.VMEM((halos, 2, nt, LANES), F32),
            pltpu.VMEM((halos, 6, nt, LANES), F32),
            pltpu.VMEM((halos, 2, SUB, LANES), F32),
            pltpu.VMEM((halos, 6, SUB, LANES), F32),
            pltpu.VMEM((halos, 4, 1, LANES), F32),
            pltpu.VMEM((halos, 12, 1, LANES), F32),
            pltpu.VMEM((halos + 1, total, 1, LANES), F32),
            pltpu.SemaphoreType.DMA((halos, 26)),
            pltpu.SemaphoreType.DMA((halos, 26)),
            pltpu.SemaphoreType.DMA((halos + 1,)),
            pltpu.SemaphoreType.DMA((halos + 1,)),
            pltpu.SemaphoreType.REGULAR((max(1, max(sizes) - 2),)),
            pltpu.VMEM((ITERS - 1, count, area), F32),
            pltpu.VMEM((ITERS - 1, count, area), F32),
            pltpu.VMEM((count, area), F32),
            pltpu.VMEM(stencils.shape[:1] + stencils.shape[4:], F32),
            pltpu.SemaphoreType.DMA((2,)),
        ],
        compiler_params=pltpu.CompilerParams(collective_id=0, has_side_effects=True, vmem_limit_bytes=48 * 1024 * 1024),
    )
    hbm = pl.BlockSpec(memory_space=pltpu.HBM)
    put = pl.pallas_call(
        store,
        out_shape=call_shapes,
        in_specs=[vmem, vmem],
        out_specs=(hbm, hbm),
        scratch_shapes=[pltpu.SemaphoreType.DMA((ITERS + 1,))],
        compiler_params=pltpu.CompilerParams(vmem_limit_bytes=4 * 1024 * 1024),
    )
    results = [put(*call(*(pltpu.with_memory_space_constraint(x, pltpu.HBM) for x in (start[0, 0, 0, p], stencils[:, 0, 0, 0])))) for p in range(probes)]
    basis = jnp.stack([r[0] for r in results])
    return basis[None, None, None], jnp.concatenate([r[1] for r in results])


def solution(mesh):
    sizes = tuple(mesh.shape[name] for name in ("gx", "gy", "gz"))
    return jax.shard_map(
        functools.partial(shards, sizes),
        mesh=mesh,
        in_specs=(P("gx", "gy", "gz", None, None, None), P(None, "gx", "gy", "gz", None, None)),
        out_specs=(P("gx", "gy", "gz", None, None, None, None), P()),
        check_vma=False,
    )
```

```python
import functools

import jax
import jax.numpy as jnp
from jax import lax
from jax.experimental import pallas as pl
from jax.experimental.pallas import tpu as pltpu
from jax.sharding import PartitionSpec as P

ITERS = 5
LANES = 128
SUB = 8
MESH = pl.DeviceIdType.MESH
F32 = jnp.float32
BF16 = jnp.bfloat16
HIGHEST = lax.Precision.HIGHEST


def iota(shape, dim):
    return lax.broadcasted_iota(jnp.int32, shape, dim)


def split(x):
    hi = x.astype(BF16)
    return hi, (x - hi.astype(F32)).astype(BF16)


def exact(a, b):
    return lax.dot_general(a, b, (((1,), (0,)), ((), ())), precision=HIGHEST, preferred_element_type=F32)


def mul(a, b):
    return jnp.dot(a, b, preferred_element_type=F32)


def swap(x):
    sub = iota((1, SUB, LANES), 1) & 3
    apart = ((iota((1, SUB, LANES), 2) >> 5) - sub) & 3
    out = x
    for d in range(1, 4):
        far = pltpu.roll(x, 32 * d, 2)
        moved = jnp.where(sub < 4 - d, pltpu.roll(far, SUB - d, 1), pltpu.roll(far, 4 - d, 1))
        out = jnp.where(apart == d, moved, out)
    return out


def build_matrices(st, mx, my, mz):
    count = st.shape[1]
    wide = LANES
    spread = ((iota((wide, count), 0) & (count - 1)) == iota((wide, count), 1)).astype(F32)
    spread_t = ((iota((count, wide), 1) & (count - 1)) == iota((count, wide), 0)).astype(F32)
    same = (iota((wide, wide), 0) >> 5) == (iota((wide, wide), 1) >> 5)
    for slot, which in ((0, 5), (1, 2)):
        big = exact(exact(spread, st[which].T), spread_t)
        hi, lo = split(jnp.where(same, big, 0.0))
        mz[0:wide, slot * wide:(slot + 1) * wide] = hi
        mz[wide:2 * wide, slot * wide:(slot + 1) * wide] = hi
        mz[2 * wide:3 * wide, slot * wide:(slot + 1) * wide] = lo
    rows = 2 * count
    r = iota((rows, count), 0)
    pick = (((r >> 3) * 4 + (r & 3)) == iota((rows, count), 1)).astype(F32)
    cols = 3 * rows
    l = iota((count, cols), 1) & (rows - 1)
    pick_t = (((l >> 3) * 4 + (l & 3)) == iota((count, cols), 0)).astype(F32)
    same = ((iota((rows, cols), 0) >> 2) & 1) == ((iota((rows, cols), 1) >> 2) & 1)
    middle = (iota((rows, cols), 1) >= rows) & (iota((rows, cols), 1) < 2 * rows)
    for slot, which in ((0, 4), (1, 1)):
        big = jnp.where(same, exact(exact(pick, st[which]), pick_t), 0.0)
        hi = big.astype(BF16).astype(F32)
        my[slot * rows:(slot + 1) * rows, :] = jnp.where(middle, big - hi, hi).astype(BF16)
    cols = 6 * count
    tile = ((iota((count, cols), 1) & (count - 1)) == iota((count, cols), 0)).astype(F32)
    stiff = exact(st[0], tile)
    mass = exact(st[3], tile)
    block = iota((count, cols), 1) >> 5
    big = jnp.where(block < 3, stiff, mass)
    hi = big.astype(BF16).astype(F32)
    mx[...] = jnp.where((block == 1) | (block == 4), big - hi, hi).astype(BF16)


def apply_patch(u, mx, my, mz):
    count, area = u.shape
    ni, nt = count // SUB, area // LANES
    tiles = jnp.concatenate(
        [u[SUB * i:SUB * (i + 1), LANES * t:LANES * (t + 1)] for i in range(ni) for t in range(nt)], axis=0
    )
    tiles = swap(tiles.reshape(ni * nt, SUB, LANES)).reshape(ni * nt * SUB, LANES)
    hi, lo = split(tiles)
    z = mul(jnp.concatenate([hi, lo, hi], axis=1), mz)
    rows = nt * SUB
    packed = []
    for slot in range(2):
        part = z[:, slot * LANES:(slot + 1) * LANES]
        wide = jnp.concatenate([part[rows * i:rows * (i + 1)] for i in range(ni)], axis=1)
        hi, lo = split(wide)
        packed.append(jnp.concatenate([hi, hi, lo], axis=0))
    both = mul(my, packed[0])
    first = both[:rows]
    second = both[rows:] + mul(my[:rows], packed[1])
    pieces = []
    for term in (first, second):
        stacked = jnp.concatenate([term[:, LANES * i:LANES * (i + 1)] for i in range(ni)], axis=0)
        stacked = swap(stacked.reshape(ni * nt, SUB, LANES))
        back = jnp.concatenate(
            [jnp.concatenate([stacked[i * nt + t] for i in range(ni)], axis=0) for t in range(nt)], axis=1
        )
        hi, lo = split(back)
        pieces += [hi, hi, lo]
    return mul(mx, jnp.concatenate(pieces, axis=0))


def kernel(sizes, start_in, st_in, basis, coef, mx, my, mz, wt, field,
           zs, zr, xs, xr, ys, yr, es, er, rows, hsend, hrecv, rsend, rrecv, ready, ws, start, st, loads):
    load_start = pltpu.make_async_copy(start_in, start, loads.at[0])
    load_st = pltpu.make_async_copy(st_in, st, loads.at[1])
    load_start.start()
    load_st.start()
    nx, ny, nz = sizes
    total = nx * ny * nz
    count, area = start.shape
    nt = area // LANES
    ni = count // SUB
    last = count - 1
    px, py, pz = lax.axis_index("gx"), lax.axis_index("gy"), lax.axis_index("gz")
    me = (px * ny + py) * nz + pz
    coords = (px, py, pz)
    there = [[coords[d] > 0, coords[d] < sizes[d] - 1] for d in range(3)]

    for ref in (zr, xr, yr, er):
        ref[...] = jnp.zeros_like(ref)
    barrier = pltpu.get_barrier_semaphore()

    def peer(k):
        p = lax.rem(me + k, total)
        return (p // (ny * nz), (p // nz) % ny, p % nz)

    def every_peer(act):
        if total > 64:
            def step(k, carry):
                act(peer(k))
                return carry

            lax.fori_loop(1, total, step, 0)
            return
        around = [[lax.rem(coords[d] + k, sizes[d]) if k else coords[d] for k in range(sizes[d])] for d in range(3)]
        for ky in range(ny - 1, -1, -1):
            for kx in range(nx - 1, -1, -1):
                for kz in range(nz):
                    if kx or ky or kz:
                        act((around[0][kx], around[1][ky], around[2][kz]))

    def neighbours(act):
        for dx in (-1, 0, 1):
            for dy in (-1, 0, 1):
                for dz in (-1, 0, 1):
                    if dx or dy or dz:
                        target = (px + dx, py + dy, pz + dz)
                        inside = None
                        for d, step in enumerate((dx, dy, dz)):
                            if step:
                                side = there[d][(step + 1) // 2]
                                inside = side if inside is None else inside & side

                        @pl.when(inside)
                        def _():
                            act(target)

    around_me = 1
    for d in range(3):
        around_me = around_me * (1 + (coords[d] > 0).astype(jnp.int32) + (coords[d] < sizes[d] - 1).astype(jnp.int32))
    around_me = around_me - 1

    rounds = max(sizes) - 2

    def call(r):
        neighbours(lambda target: pl.semaphore_signal(ready.at[r], inc=1, device_id=target, device_id_type=MESH))

    neighbours(lambda target: pl.semaphore_signal(barrier, inc=1, device_id=target, device_id_type=MESH))

    def shared(index, d):
        return ((index == 0) & there[d][0]) | ((index == last) & there[d][1])

    lane = iota((count, area), 1)
    ia, ib, ic = iota((count, area), 0), lane >> 5, lane & (count - 1)
    half = lambda index, d: jnp.where(shared(index, d), 0.5, 1.0)
    weight = half(ia, 0) * half(ib, 1) * half(ic, 2)
    wt[...] = weight.astype(F32)
    load_start.wait()
    field[...] = start[...] * wt[...]

    lane_c = iota((count, LANES), 1)
    face_c = (lane_c & (count - 1) == 0) | (lane_c & (count - 1) == last)
    even = (lane_c & 1) == 0
    lane8 = iota((SUB, LANES), 1)
    low8, high8 = lane8 < count, lane8 >= LANES - count
    lane1 = iota((1, LANES), 1)
    diag = iota((SUB, LANES), 0) == lane8

    def tile(t):
        return slice(t * LANES, (t + 1) * LANES)

    def halo_copies(phase):
        out = []

        def add(src, dst, slot, *direction):
            there_all, target = None, {}
            for d, step in enumerate(direction):
                if step is not None:
                    there_all = there[d][step] if there_all is None else there_all & there[d][step]
            target = tuple(c if step is None else c + 2 * step - 1 for c, step in zip(coords, direction))
            copy = pltpu.make_async_remote_copy(
                src_ref=src, dst_ref=dst.at[phase, slot], send_sem=hsend.at[phase, len(out)],
                recv_sem=hrecv.at[phase, len(out)], device_id=target, device_id_type=MESH)
            out.append((copy, there_all, direction, dst, slot))

        for z in (None, 1, 0):
            for d in range(2):
                for e in range(2):
                    back = 0 if z is None else 2 - z
                    add(es.at[phase, 2 * d + e], er, (2 * (1 - d) + 1 - e) * 3 + back, d, e, z)
        for z in (None, 1, 0):
            back = 0 if z is None else 2 - z
            for d in range(2):
                add(xs.at[phase, d], xr, (1 - d) * 3 + back, d, None, z)
        for z in (None, 1, 0):
            back = 0 if z is None else 2 - z
            for d in range(2):
                add(ys.at[phase, d], yr, (1 - d) * 3 + back, None, d, z)
        for d in range(2):
            add(zs.at[phase], zr, 1 - d, None, None, d)
        return out

    def start_all(copies):
        for copy, exists, *_ in copies:
            @pl.when(exists)
            def _():
                copy.start()

    def send_halo(phase):
        copies = halo_copies(phase)
        for d in range(2):
            row = 0 if d == 0 else last
            for e in range(2):
                es[phase, 2 * d + e] = field[row:row + 1, tile(0 if e == 0 else nt - 1)]
            for t in range(nt):
                xs[phase, d, t:t + 1, :] = field[row:row + 1, tile(t)]
            packed = None
            for i in range(ni):
                block = field[SUB * i:SUB * (i + 1), tile(0 if d == 0 else nt - 1)]
                part = jnp.where(low8 if d == 0 else high8, block, 0.0)
                shift = (count * i + d * count) % LANES
                part = part if shift == 0 else pltpu.roll(part, shift, 1)
                packed = part if packed is None else packed + part
            ys[phase, d] = packed
        packed = None
        for t in range(nt):
            part = jnp.where(face_c, field[:, tile(t)], 0.0)
            part = part if t == 0 else pltpu.roll(part, 2 * t, 1)
            packed = part if packed is None else packed + part
        zs[phase] = packed
        start_all(copies)

    def fold(ref, phase, base, shift=0):
        low = ref[phase, base + 1]
        c = iota(low.shape, 1) & (count - 1)
        turn = lambda x, by: x if by % LANES == 0 else pltpu.roll(x, by % LANES, 1)
        out = turn(ref[phase, base], shift) + jnp.where(c == 0, turn(low, shift - last), 0.0)
        return out + jnp.where(c == last, turn(ref[phase, base + 2], shift + last), 0.0)

    def add_halo(phase):
        copies = halo_copies(phase)
        for index, (copy, _, direction, dst, slot) in enumerate(copies):
            mirror = None
            for d, step in enumerate(direction):
                if step is not None:
                    mirror = there[d][1 - step] if mirror is None else mirror & there[d][1 - step]

            @pl.when(mirror)
            def _():
                into = dst.at[phase, slot]
                pltpu.make_async_copy(into, into, hrecv.at[phase, index]).wait()
        merged = jnp.where(even, pltpu.roll(zr[phase, 0], LANES - last, 1), pltpu.roll(zr[phase, 1], last, 1))
        for t in range(nt):
            part = merged if t == 0 else pltpu.roll(merged, LANES - 2 * t, 1)
            field[:, tile(t)] += jnp.where(face_c, part, 0.0)
        for d in range(2):
            received = fold(yr, phase, 3 * d)
            for i in range(ni):
                shift = (-count * i - d * count) % LANES
                part = received if shift == 0 else pltpu.roll(received, shift, 1)
                field[SUB * i:SUB * (i + 1), tile(0 if d == 0 else nt - 1)] += jnp.where(low8 if d == 0 else high8, part, 0.0)
        for d in range(2):
            row = 0 if d == 0 else last
            received = fold(xr, phase, 3 * d)
            for t in range(nt):
                line = received[t:t + 1]
                if t == 0:
                    line += jnp.where(lane1 < count, fold(er, phase, 6 * d, count), 0.0)
                if t == nt - 1:
                    line += jnp.where(lane1 >= LANES - count, fold(er, phase, 6 * d + 3, LANES - count), 0.0)
                field[row:row + 1, tile(t)] += line

    def send_dots(phase, products):
        packed = None
        for k, product in enumerate(products):
            acc = None
            for i in range(ni):
                for t in range(nt):
                    block = product[SUB * i:SUB * (i + 1), tile(t)]
                    acc = block if acc is None else acc + block
            line = jnp.where(iota((SUB, LANES), 0) == k, jnp.sum(acc, axis=0, keepdims=True), 0.0)
            packed = line if packed is None else packed + line
        sums = jnp.sum(packed, axis=1, keepdims=True)
        rows[phase, me] = jnp.sum(jnp.where(diag, sums, 0.0), axis=0, keepdims=True)

        def send(target):
            pltpu.make_async_remote_copy(
                src_ref=rows.at[phase, me], dst_ref=rows.at[phase, me], send_sem=rsend.at[phase],
                recv_sem=rrecv.at[phase], device_id=target, device_id_type=MESH).start()

        every_peer(send)

    def take_dots(phase):
        others = rows.at[phase, pl.ds(0, total - 1)]
        pltpu.make_async_copy(others, others, rrecv.at[phase]).wait()
        line = jnp.sum(rows[phase], axis=0)
        return jnp.sum(jnp.where(diag, line, 0.0), axis=1, keepdims=True)

    pl.semaphore_wait(barrier, around_me)
    send_halo(0)
    load_st.wait()
    build_matrices(st, mx, my, mz)
    for r in range(rounds):
        call(r)
        if r < rounds - 1:
            pl.semaphore_wait(ready.at[r], around_me)
    add_halo(0)
    ws[0] = field[...]
    gram, rho = {}, [None]

    def gather(k):
        sums = take_dots(k)
        for i in range(k + 1):
            gram[i, k] = sums[i:i + 1]
        if k < ITERS:
            rho.append(sums[k + 1:k + 2] / sums[k:k + 1])

    for k in range(ITERS):
        vector = ws[k]
        local = apply_patch(vector, mx[...], my[...], mz[...])
        field[...] = local
        send_halo(k + 1)
        if k == 0 and rounds > 0:
            pl.semaphore_wait(ready.at[rounds - 1], around_me)
        weighted = wt[...] * vector
        send_dots(k, [weighted * ws[i] for i in range(k + 1)] + [local * vector])
        if k > 0:
            gather(k - 1)
        add_halo(k + 1)
        ws[k + 1] = field[...] if k == 0 else field[...] * (1.0 / rho[k]) - vector
    weighted = wt[...] * ws[ITERS]
    send_dots(ITERS, [weighted * ws[i] for i in range(ITERS + 1)])
    gather(ITERS - 1)

    upper, inverse, scale = {}, {}, []

    def column(k):
        for i in range(k):
            total_i = None
            for m in range(i + 1):
                term = inverse[m, i] * gram[m, k]
                total_i = term if total_i is None else total_i + term
            upper[i, k] = total_i
        rest = gram[k, k]
        for i in range(k):
            rest = rest - upper[i, k] * upper[i, k]
        upper[k, k] = jnp.sqrt(rest)
        inverse[k, k] = 1.0 / upper[k, k]
        for i in range(k):
            total_i = None
            for m in range(i, k):
                term = inverse[i, m] * upper[m, k]
                total_i = term if total_i is None else total_i + term
            inverse[i, k] = -total_i * inverse[k, k]
        if k > 0:
            out = ws[0] * inverse[0, k]
            for i in range(1, k + 1):
                out = out + ws[i] * inverse[i, k]
            basis[k - 1] = out

    for k in range(ITERS):
        column(k)
    gather(ITERS)
    column(ITERS)
    row2, col2 = iota(coef.shape[1:], 0), iota(coef.shape[1:], 1)
    coefs = jnp.zeros(coef.shape[1:], F32)
    for k in range(ITERS):
        step = 1.0 if k == 0 else rho[k]
        alpha = step * (upper[k, k + 1] * inverse[k, k])
        if k > 0:
            alpha = alpha + rho[k]
            alpha = alpha - (1.0 if k == 1 else rho[k - 1]) * (upper[k - 1, k] * inverse[k - 1, k - 1])
        beta = step * (upper[k + 1, k + 1] * inverse[k, k])
        coefs = jnp.where((row2 == 0) & (col2 == k), alpha, coefs)
        coefs = jnp.where((row2 == 1) & (col2 == k), beta, coefs)
    coef[0] = coefs

    for phase in range(ITERS + 1):
        for copy, exists, *_ in halo_copies(phase):
            @pl.when(exists)
            def _():
                copy.wait_send()
    for phase in range(ITERS + 1):
        others = rows.at[phase, pl.ds(0, total - 1)]
        pltpu.make_async_copy(others, others, rsend.at[phase]).wait()


def store(basis, coef, basis_out, coef_out, sems):
    copies = [pltpu.make_async_copy(basis.at[i], basis_out.at[i], sems.at[i]) for i in range(ITERS)]
    copies.append(pltpu.make_async_copy(coef, coef_out, sems.at[ITERS]))
    for copy in copies:
        copy.start()
    for copy in copies:
        copy.wait()


def shards(sizes, start, stencils):
    probes, count, area = start.shape[3:]
    nt = area // LANES
    total = sizes[0] * sizes[1] * sizes[2]
    halos = ITERS + 1
    vmem = pl.BlockSpec(memory_space=pltpu.VMEM)
    call_shapes = (jax.ShapeDtypeStruct((ITERS, count, area), F32), jax.ShapeDtypeStruct((1, 2, ITERS), F32))
    call = pl.pallas_call(
        functools.partial(kernel, sizes),
        out_shape=call_shapes,
        in_specs=[pl.BlockSpec(memory_space=pltpu.HBM)] * 2,
        out_specs=(vmem, vmem),
        scratch_shapes=[
            pltpu.VMEM((count, 6 * count), BF16),
            pltpu.VMEM((4 * count, 6 * count), BF16),
            pltpu.VMEM((3 * LANES, 2 * LANES), BF16),
            pltpu.VMEM((count, area), F32),
            pltpu.VMEM((count, area), F32),
            pltpu.VMEM((halos, count, LANES), F32),
            pltpu.VMEM((halos, 2, count, LANES), F32),
            pltpu.VMEM((halos, 2, nt, LANES), F32),
            pltpu.VMEM((halos, 6, nt, LANES), F32),
            pltpu.VMEM((halos, 2, SUB, LANES), F32),
            pltpu.VMEM((halos, 6, SUB, LANES), F32),
            pltpu.VMEM((halos, 4, 1, LANES), F32),
            pltpu.VMEM((halos, 12, 1, LANES), F32),
            pltpu.VMEM((halos, total, 1, LANES), F32),
            pltpu.SemaphoreType.DMA((halos, 26)),
            pltpu.SemaphoreType.DMA((halos, 26)),
            pltpu.SemaphoreType.DMA((halos,)),
            pltpu.SemaphoreType.DMA((halos,)),
            pltpu.SemaphoreType.REGULAR((max(1, max(sizes) - 2),)),
            pltpu.VMEM((halos, count, area), F32),
            pltpu.VMEM((count, area), F32),
            pltpu.VMEM(stencils.shape[:1] + stencils.shape[4:], F32),
            pltpu.SemaphoreType.DMA((2,)),
        ],
        compiler_params=pltpu.CompilerParams(collective_id=0, has_side_effects=True, vmem_limit_bytes=48 * 1024 * 1024),
    )
    hbm = pl.BlockSpec(memory_space=pltpu.HBM)
    put = pl.pallas_call(
        store,
        out_shape=call_shapes,
        in_specs=[vmem, vmem],
        out_specs=(hbm, hbm),
        scratch_shapes=[pltpu.SemaphoreType.DMA((ITERS + 1,))],
        compiler_params=pltpu.CompilerParams(vmem_limit_bytes=4 * 1024 * 1024),
    )
    results = [put(*call(*(pltpu.with_memory_space_constraint(x, pltpu.HBM) for x in (start[0, 0, 0, p], stencils[:, 0, 0, 0])))) for p in range(probes)]
    basis = jnp.stack([r[0] for r in results])
    return basis[None, None, None], jnp.concatenate([r[1] for r in results])


def solution(mesh):
    sizes = tuple(mesh.shape[name] for name in ("gx", "gy", "gz"))
    return jax.shard_map(
        functools.partial(shards, sizes),
        mesh=mesh,
        in_specs=(P("gx", "gy", "gz", None, None, None), P(None, "gx", "gy", "gz", None, None)),
        out_specs=(P("gx", "gy", "gz", None, None, None, None), P()),
        check_vma=False,
    )
```

```python
import functools

import jax
import jax.numpy as jnp
from jax import lax
from jax.experimental import pallas as pl
from jax.experimental.pallas import tpu as pltpu
from jax.sharding import PartitionSpec as P

ITERS = 5
LANES = 128
SUB = 8
MESH = pl.DeviceIdType.MESH
F32 = jnp.float32
BF16 = jnp.bfloat16
HIGHEST = lax.Precision.HIGHEST


def iota(shape, dim):
    return lax.broadcasted_iota(jnp.int32, shape, dim)


def split(x):
    hi = x.astype(BF16)
    return hi, (x - hi.astype(F32)).astype(BF16)


def exact(a, b):
    return lax.dot_general(a, b, (((1,), (0,)), ((), ())), precision=HIGHEST, preferred_element_type=F32)


def mul(a, b):
    return jnp.dot(a, b, preferred_element_type=F32)


def swap(x):
    sub = iota((1, SUB, LANES), 1) & 3
    apart = ((iota((1, SUB, LANES), 2) >> 5) - sub) & 3
    out = x
    for d in range(1, 4):
        far = pltpu.roll(x, 32 * d, 2)
        moved = jnp.where(sub < 4 - d, pltpu.roll(far, SUB - d, 1), pltpu.roll(far, 4 - d, 1))
        out = jnp.where(apart == d, moved, out)
    return out


def build_matrices(st, mx, my, mz, mzt, ya, yb):
    count = st.shape[1]
    wide = LANES
    spread = ((iota((wide, count), 0) & (count - 1)) == iota((wide, count), 1)).astype(F32)
    spread_t = ((iota((count, wide), 1) & (count - 1)) == iota((count, wide), 0)).astype(F32)
    same = (iota((wide, wide), 0) >> 5) == (iota((wide, wide), 1) >> 5)
    for slot, which in ((0, 5), (1, 2)):
        big = exact(exact(spread, st[which].T), spread_t)
        for ref, values in ((mz, jnp.where(same, big, 0.0)), (mzt, big)):
            hi, lo = split(values)
            ref[0:wide, slot * wide:(slot + 1) * wide] = hi
            ref[wide:2 * wide, slot * wide:(slot + 1) * wide] = hi
            ref[2 * wide:3 * wide, slot * wide:(slot + 1) * wide] = lo
    rows = 2 * count
    r = iota((rows, count), 0)
    pick = (((r >> 3) * 4 + (r & 3)) == iota((rows, count), 1)).astype(F32)
    cols = 3 * rows
    l = iota((count, cols), 1) & (rows - 1)
    pick_t = (((l >> 3) * 4 + (l & 3)) == iota((count, cols), 0)).astype(F32)
    same = ((iota((rows, cols), 0) >> 2) & 1) == ((iota((rows, cols), 1) >> 2) & 1)
    middle = (iota((rows, cols), 1) >= rows) & (iota((rows, cols), 1) < 2 * rows)
    for slot, which in ((0, 4), (1, 1)):
        big = jnp.where(same, exact(exact(pick, st[which]), pick_t), 0.0)
        hi = big.astype(BF16).astype(F32)
        my[slot * rows:(slot + 1) * rows, :] = jnp.where(middle, big - hi, hi).astype(BF16)
    cols = 7 * count
    row, col = iota((count, cols), 0), iota((count, cols), 1)
    block, extra, part = col >> 5, col >= 6 * count, (col >> 3) & 3
    source = jnp.where(extra, jnp.where((col & 2) == 0, 0, count - 1), col & (count - 1))
    tile = (source == row).astype(F32)
    big = jnp.where((extra & ((col & 4) == 0)) | (~extra & (block >= 3)), exact(st[3], tile), exact(st[0], tile))
    hi = big.astype(BF16).astype(F32)
    rest = (~extra & ((block == 1) | (block == 4))) | (extra & (part == 1))
    mx[...] = jnp.where(extra & (part == 3), 0.0, jnp.where(rest, big - hi, hi)).astype(BF16)
    r, b = iota((SUB, count), 0), iota((SUB, count), 1)
    ends = (b == jnp.where((r & 1) == 0, 0, count - 1)).astype(F32)
    area = ya.shape[1]
    widen = ((iota((count, area), 1) >> 5) == iota((count, area), 0)).astype(F32)
    mass = exact(exact(ends, st[4].T), widen)
    stiff = exact(exact(ends, st[1].T), widen)
    upper = iota((SUB, area), 0) < SUB // 2
    ya[...] = jnp.where(upper, stiff, mass)
    yb[...] = jnp.where(upper, mass, 0.0)


def apply_patch(u, mx, my, mz, late, send):
    count, area = u.shape
    ni, nt = count // SUB, area // LANES
    rows = nt * SUB
    terms = []
    for h in range(2):
        group = range(h * ni // 2, (h + 1) * ni // 2)
        tiles = jnp.concatenate([u[SUB * i:SUB * (i + 1), LANES * t:LANES * (t + 1)] for i in group for t in range(nt)], axis=0)
        tiles = swap(tiles.reshape(-1, SUB, LANES)).reshape(-1, LANES)
        hi, lo = split(tiles)
        z = mul(jnp.concatenate([hi, lo, hi], axis=1), mz)
        packed = []
        for slot in range(2):
            part = z[:, slot * LANES:(slot + 1) * LANES]
            wide = jnp.concatenate([part[rows * i:rows * (i + 1)] for i in range(len(group))], axis=1)
            hi, lo = split(wide)
            packed.append(jnp.concatenate([hi, hi, lo], axis=0))
        both = mul(my, packed[0])
        terms.append((both[:rows], both[rows:] + mul(my[:rows], packed[1])))
    lines = late()
    half = ni // 2
    order = [0, nt - 1] + list(range(1, nt - 1))
    for at in range(0, nt, 2):
        pair = order[at:at + 2]
        stacked = jnp.stack([
            terms[i // half][k][SUB * t:SUB * (t + 1), LANES * (i % half):LANES * (i % half + 1)]
            for k in range(2) for t in pair for i in range(ni)
        ])
        stacked = swap(stacked)
        pieces = []
        for k in range(2):
            back = jnp.concatenate([
                jnp.concatenate([stacked[(k * 2 + n) * ni + i] for i in range(ni)], axis=0) for n in range(2)
            ], axis=1)
            hi, lo = split(back)
            pieces += [hi, hi, lo]
        pieces.append(jnp.concatenate([lines[t] for t in pair], axis=1))
        out = mul(mx, jnp.concatenate(pieces, axis=0))
        send({t: out[:, LANES * n:LANES * (n + 1)] for n, t in enumerate(pair)}, at == 0)


def kernel(sizes, start_in, st_in, basis, coef, mx, my, mz, mzt, ya, yb, wt, field,
           zs, zr, xs, xr, ys, yr, es, er, rows, hsend, hrecv, rsend, rrecv, ready, ws, start, st, loads):
    load_start = pltpu.make_async_copy(start_in, start, loads.at[0])
    load_st = pltpu.make_async_copy(st_in, st, loads.at[1])
    load_start.start()
    load_st.start()
    nx, ny, nz = sizes
    total = nx * ny * nz
    count, area = start.shape
    nt = area // LANES
    ni = count // SUB
    last = count - 1
    px, py, pz = lax.axis_index("gx"), lax.axis_index("gy"), lax.axis_index("gz")
    me = (px * ny + py) * nz + pz
    coords = (px, py, pz)
    there = [[coords[d] > 0, coords[d] < sizes[d] - 1] for d in range(3)]

    for ref in (zr, xr, yr, er):
        ref[...] = jnp.zeros_like(ref)
    barrier = pltpu.get_barrier_semaphore()

    def peer(k):
        p = lax.rem(me + k, total)
        return (p // (ny * nz), (p // nz) % ny, p % nz)

    def every_peer(act):
        if total > 64:
            def step(k, carry):
                act(peer(k))
                return carry

            lax.fori_loop(1, total, step, 0)
            return
        around = [[lax.rem(coords[d] + k, sizes[d]) if k else coords[d] for k in range(sizes[d])] for d in range(3)]
        for ky in range(ny - 1, -1, -1):
            for kx in range(nx - 1, -1, -1):
                for kz in range(nz):
                    if kx or ky or kz:
                        act((around[0][kx], around[1][ky], around[2][kz]))

    def neighbours(act):
        for dx in (-1, 0, 1):
            for dy in (-1, 0, 1):
                for dz in (-1, 0, 1):
                    if dx or dy or dz:
                        target = (px + dx, py + dy, pz + dz)
                        inside = None
                        for d, step in enumerate((dx, dy, dz)):
                            if step:
                                side = there[d][(step + 1) // 2]
                                inside = side if inside is None else inside & side

                        @pl.when(inside)
                        def _():
                            act(target)

    around_me = 1
    for d in range(3):
        around_me = around_me * (1 + (coords[d] > 0).astype(jnp.int32) + (coords[d] < sizes[d] - 1).astype(jnp.int32))
    around_me = around_me - 1

    rounds = max(sizes) - 2

    def call(r):
        neighbours(lambda target: pl.semaphore_signal(ready.at[r], inc=1, device_id=target, device_id_type=MESH))

    neighbours(lambda target: pl.semaphore_signal(barrier, inc=1, device_id=target, device_id_type=MESH))

    def shared(index, d):
        return ((index == 0) & there[d][0]) | ((index == last) & there[d][1])

    lane = iota((count, area), 1)
    ia, ib, ic = iota((count, area), 0), lane >> 5, lane & (count - 1)
    half = lambda index, d: jnp.where(shared(index, d), 0.5, 1.0)
    weight = half(ia, 0) * half(ib, 1) * half(ic, 2)
    wt[...] = weight.astype(F32)
    load_start.wait()
    field[...] = start[...] * wt[...]

    lane_c = iota((count, LANES), 1)
    face_c = (lane_c & (count - 1) == 0) | (lane_c & (count - 1) == last)
    even = (lane_c & 1) == 0
    lane8 = iota((SUB, LANES), 1)
    low8, high8 = lane8 < count, lane8 >= LANES - count
    lane1 = iota((1, LANES), 1)
    diag = iota((SUB, LANES), 0) == lane8

    def tile(t):
        return slice(t * LANES, (t + 1) * LANES)

    def halo_copies(phase):
        out = []

        def add(src, into, *direction):
            there_all, target = None, {}
            for d, step in enumerate(direction):
                if step is not None:
                    there_all = there[d][step] if there_all is None else there_all & there[d][step]
            target = tuple(c if step is None else c + 2 * step - 1 for c, step in zip(coords, direction))
            copy = pltpu.make_async_remote_copy(
                src_ref=src, dst_ref=into, send_sem=hsend.at[phase, len(out)],
                recv_sem=hrecv.at[phase, len(out)], device_id=target, device_id_type=MESH)
            out.append((copy, there_all, direction, into))

        for z in (None, 1, 0):
            for d in range(2):
                for e in range(2):
                    back = 0 if z is None else 2 - z
                    add(es.at[phase, 2 * d + e], er.at[phase, back, pl.ds(2 * (1 - d) + 1 - e, 1)], d, e, z)
        for z in (None, 1, 0):
            back = 0 if z is None else 2 - z
            for d in range(2):
                add(xs.at[phase, d], xr.at[phase, (1 - d) * 3 + back], d, None, z)
        for z in (None, 1, 0):
            back = 0 if z is None else 2 - z
            for d in range(2):
                add(ys.at[phase, d], yr.at[phase, (1 - d) * 3 + back], None, d, z)
        for d in range(2):
            add(zs.at[phase], zr.at[phase, 1 - d], None, None, d)
        return out

    def start_all(copies):
        for copy, exists, *_ in copies:
            @pl.when(exists)
            def _():
                copy.start()

    def send_halo(phase):
        copies = halo_copies(phase)

        def send(local, first):
            for t, value in local.items():
                field[:, tile(t)] = value
            for d in range(2):
                row = 0 if d == 0 else last
                for t, value in local.items():
                    xs[phase, d, t:t + 1, :] = value[row:row + 1]
                if first:
                    for e in range(2):
                        es[phase, 2 * d + e] = local[0 if e == 0 else nt - 1][row:row + 1]
            if not first:
                return
            start_all(copies[:12])
            for d in range(2):
                packed = None
                for i in range(ni):
                    block = local[0 if d == 0 else nt - 1][SUB * i:SUB * (i + 1)]
                    part = jnp.where(low8 if d == 0 else high8, block, 0.0)
                    shift = (count * i + d * count) % LANES
                    part = part if shift == 0 else pltpu.roll(part, shift, 1)
                    packed = part if packed is None else packed + part
                ys[phase, d] = packed

        def rest():
            start_all(copies[12:24])
            packed = None
            for t in range(nt):
                part = jnp.where(face_c, field[:, tile(t)], 0.0)
                part = part if t == 0 else pltpu.roll(part, 2 * t, 1)
                packed = part if packed is None else packed + part
            zs[phase] = packed
            start_all(copies[24:])

        return send, rest

    def fold(ref, phase, base, shift=0):
        low = ref[phase, base + 1]
        c = iota(low.shape, 1) & (count - 1)
        turn = lambda x, by: x if by % LANES == 0 else pltpu.roll(x, by % LANES, 1)
        out = turn(ref[phase, base], shift) + jnp.where(c == 0, turn(low, shift - last), 0.0)
        return out + jnp.where(c == last, turn(ref[phase, base + 2], shift + last), 0.0)

    def arrive(phase, chosen):
        copies = halo_copies(phase)
        for index in chosen:
            _, _, direction, into = copies[index]
            mirror = None
            for d, step in enumerate(direction):
                if step is not None:
                    mirror = there[d][1 - step] if mirror is None else mirror & there[d][1 - step]

            @pl.when(mirror)
            def _():
                pltpu.make_async_copy(into, into, hrecv.at[phase, index]).wait()

    def add_faces(phase):
        arrive(phase, range(24, 26))
        merged = jnp.where(even, pltpu.roll(zr[phase, 0], LANES - last, 1), pltpu.roll(zr[phase, 1], last, 1))
        for t in range(nt):
            part = merged if t == 0 else pltpu.roll(merged, LANES - 2 * t, 1)
            field[:, tile(t)] += jnp.where(face_c, part, 0.0)
        arrive(phase, range(18, 24))
        for d in range(2):
            received = fold(yr, phase, 3 * d)
            for i in range(ni):
                shift = (-count * i - d * count) % LANES
                part = received if shift == 0 else pltpu.roll(received, shift, 1)
                field[SUB * i:SUB * (i + 1), tile(0 if d == 0 else nt - 1)] += jnp.where(low8 if d == 0 else high8, part, 0.0)
        arrive(phase, range(12, 18))
        for d in range(2):
            row = 0 if d == 0 else last
            received = fold(xr, phase, 3 * d)
            for t in range(nt):
                field[row:row + 1, tile(t)] += received[t:t + 1]

    def take_edges(phase, factor):
        arrive(phase, range(12))
        c = lane8 & (count - 1)
        out = er[phase, 0] + jnp.where(c == 0, pltpu.roll(er[phase, 1], LANES - last, 1), 0.0)
        out = out + jnp.where(c == last, pltpu.roll(er[phase, 2], last, 1), 0.0)
        side = (iota((SUB, LANES), 0) & 1) == 0
        out = jnp.where((side & high8) | (~side & low8), out, 0.0)
        return out if factor is None else out * factor

    def lines_of(edges):
        twice = edges + pltpu.roll(edges, SUB // 2, 0)
        twice = jnp.concatenate([twice, jnp.zeros_like(twice)], axis=0)
        hi, lo = split(twice)
        z = mul(jnp.concatenate([hi, lo, hi], axis=1), mzt[...])[:SUB]
        out = []
        for t in range(nt):
            line = ya[:, tile(t)] * z[:, :LANES] + yb[:, tile(t)] * z[:, LANES:]
            hi = line.astype(BF16).astype(F32)
            out.append(jnp.concatenate([hi, hi, line - hi, jnp.zeros_like(hi)], axis=0).astype(BF16))
        return out

    def add_edges(k, edges):
        for d in range(2):
            row = 0 if d == 0 else last
            ws[k, row:row + 1, tile(0)] += pltpu.roll(edges[2 * d:2 * d + 1], count, 1)
            ws[k, row:row + 1, tile(nt - 1)] += pltpu.roll(edges[2 * d + 1:2 * d + 2], LANES - count, 1)

    def send_dots(phase, products):
        packed = None
        for k, product in enumerate(products):
            acc = None
            for i in range(ni):
                for t in range(nt):
                    block = product[SUB * i:SUB * (i + 1), tile(t)]
                    acc = block if acc is None else acc + block
            line = jnp.where(iota((SUB, LANES), 0) == k, jnp.sum(acc, axis=0, keepdims=True), 0.0)
            packed = line if packed is None else packed + line
        sums = jnp.sum(packed, axis=1, keepdims=True)
        rows[phase, me] = jnp.sum(jnp.where(diag, sums, 0.0), axis=0, keepdims=True)

        def send(target):
            pltpu.make_async_remote_copy(
                src_ref=rows.at[phase, me], dst_ref=rows.at[phase, me], send_sem=rsend.at[phase],
                recv_sem=rrecv.at[phase], device_id=target, device_id_type=MESH).start()

        every_peer(send)

    def take_dots(phase):
        others = rows.at[phase, pl.ds(0, total - 1)]
        pltpu.make_async_copy(others, others, rrecv.at[phase]).wait()
        line = jnp.sum(rows[phase], axis=0)
        return jnp.sum(jnp.where(diag, line, 0.0), axis=1, keepdims=True)

    pl.semaphore_wait(barrier, around_me)
    send, rest = send_halo(0)
    value = field[...]
    send({t: value[:, tile(t)] for t in range(nt)}, True)
    rest()
    load_st.wait()
    build_matrices(st, mx, my, mz, mzt, ya, yb)
    for r in range(rounds):
        call(r)
        if r < rounds - 1:
            pl.semaphore_wait(ready.at[r], around_me)
    add_faces(0)
    ws[0] = field[...]
    gram, rho = {}, [None]

    def gather(k):
        sums = take_dots(k)
        for i in range(k + 1):
            gram[i, k] = sums[i:i + 1]
        if k < ITERS:
            rho.append(sums[k + 1:k + 2] / sums[k:k + 1])

    factor = None
    for k in range(ITERS):
        edges = []

        def late():
            edges.append(take_edges(k, factor))
            return lines_of(edges[0])

        send, rest = send_halo(k + 1)
        apply_patch(ws[k], mx[...], my[...], mz[...], late, send)
        rest()
        if k == 0 and rounds > 0:
            pl.semaphore_wait(ready.at[rounds - 1], around_me)
        add_edges(k, edges[0])
        vector = ws[k]
        weighted = wt[...] * vector
        send_dots(k, [weighted * ws[i] for i in range(k + 1)] + [field[...] * vector])
        if k > 0:
            gather(k - 1)
            factor = 1.0 / rho[k]
        add_faces(k + 1)
        ws[k + 1] = field[...] if k == 0 else field[...] * factor - vector
    add_edges(ITERS, take_edges(ITERS, factor))
    weighted = wt[...] * ws[ITERS]
    send_dots(ITERS, [weighted * ws[i] for i in range(ITERS + 1)])
    gather(ITERS - 1)

    upper, inverse, scale = {}, {}, []

    def column(k):
        for i in range(k):
            total_i = None
            for m in range(i + 1):
                term = inverse[m, i] * gram[m, k]
                total_i = term if total_i is None else total_i + term
            upper[i, k] = total_i
        rest = gram[k, k]
        for i in range(k):
            rest = rest - upper[i, k] * upper[i, k]
        upper[k, k] = jnp.sqrt(rest)
        inverse[k, k] = 1.0 / upper[k, k]
        for i in range(k):
            total_i = None
            for m in range(i, k):
                term = inverse[i, m] * upper[m, k]
                total_i = term if total_i is None else total_i + term
            inverse[i, k] = -total_i * inverse[k, k]
        if k > 0:
            out = ws[0] * inverse[0, k]
            for i in range(1, k + 1):
                out = out + ws[i] * inverse[i, k]
            basis[k - 1] = out

    for k in range(ITERS):
        column(k)
    gather(ITERS)
    column(ITERS)
    row2, col2 = iota(coef.shape[1:], 0), iota(coef.shape[1:], 1)
    coefs = jnp.zeros(coef.shape[1:], F32)
    for k in range(ITERS):
        step = 1.0 if k == 0 else rho[k]
        alpha = step * (upper[k, k + 1] * inverse[k, k])
        if k > 0:
            alpha = alpha + rho[k]
            alpha = alpha - (1.0 if k == 1 else rho[k - 1]) * (upper[k - 1, k] * inverse[k - 1, k - 1])
        beta = step * (upper[k + 1, k + 1] * inverse[k, k])
        coefs = jnp.where((row2 == 0) & (col2 == k), alpha, coefs)
        coefs = jnp.where((row2 == 1) & (col2 == k), beta, coefs)
    coef[0] = coefs

    for phase in range(ITERS + 1):
        for copy, exists, *_ in halo_copies(phase):
            @pl.when(exists)
            def _():
                copy.wait_send()
    for phase in range(ITERS + 1):
        others = rows.at[phase, pl.ds(0, total - 1)]
        pltpu.make_async_copy(others, others, rsend.at[phase]).wait()


def store(basis, coef, basis_out, coef_out, sems):
    copies = [pltpu.make_async_copy(basis.at[i], basis_out.at[i], sems.at[i]) for i in range(ITERS)]
    copies.append(pltpu.make_async_copy(coef, coef_out, sems.at[ITERS]))
    for copy in copies:
        copy.start()
    for copy in copies:
        copy.wait()


def shards(sizes, start, stencils):
    probes, count, area = start.shape[3:]
    nt = area // LANES
    total = sizes[0] * sizes[1] * sizes[2]
    halos = ITERS + 1
    vmem = pl.BlockSpec(memory_space=pltpu.VMEM)
    call_shapes = (jax.ShapeDtypeStruct((ITERS, count, area), F32), jax.ShapeDtypeStruct((1, 2, ITERS), F32))
    call = pl.pallas_call(
        functools.partial(kernel, sizes),
        out_shape=call_shapes,
        in_specs=[pl.BlockSpec(memory_space=pltpu.HBM)] * 2,
        out_specs=(vmem, vmem),
        scratch_shapes=[
            pltpu.VMEM((count, 7 * count), BF16),
            pltpu.VMEM((4 * count, 6 * count), BF16),
            pltpu.VMEM((3 * LANES, 2 * LANES), BF16),
            pltpu.VMEM((3 * LANES, 2 * LANES), BF16),
            pltpu.VMEM((SUB, area), F32),
            pltpu.VMEM((SUB, area), F32),
            pltpu.VMEM((count, area), F32),
            pltpu.VMEM((count, area), F32),
            pltpu.VMEM((halos, count, LANES), F32),
            pltpu.VMEM((halos, 2, count, LANES), F32),
            pltpu.VMEM((halos, 2, nt, LANES), F32),
            pltpu.VMEM((halos, 6, nt, LANES), F32),
            pltpu.VMEM((halos, 2, SUB, LANES), F32),
            pltpu.VMEM((halos, 6, SUB, LANES), F32),
            pltpu.VMEM((halos, 4, 1, LANES), F32),
            pltpu.VMEM((halos, 3, SUB, LANES), F32),
            pltpu.VMEM((halos, total, 1, LANES), F32),
            pltpu.SemaphoreType.DMA((halos, 26)),
            pltpu.SemaphoreType.DMA((halos, 26)),
            pltpu.SemaphoreType.DMA((halos,)),
            pltpu.SemaphoreType.DMA((halos,)),
            pltpu.SemaphoreType.REGULAR((max(1, max(sizes) - 2),)),
            pltpu.VMEM((halos, count, area), F32),
            pltpu.VMEM((count, area), F32),
            pltpu.VMEM(stencils.shape[:1] + stencils.shape[4:], F32),
            pltpu.SemaphoreType.DMA((2,)),
        ],
        compiler_params=pltpu.CompilerParams(collective_id=0, has_side_effects=True, vmem_limit_bytes=48 * 1024 * 1024),
    )
    hbm = pl.BlockSpec(memory_space=pltpu.HBM)
    put = pl.pallas_call(
        store,
        out_shape=call_shapes,
        in_specs=[vmem, vmem],
        out_specs=(hbm, hbm),
        scratch_shapes=[pltpu.SemaphoreType.DMA((ITERS + 1,))],
        compiler_params=pltpu.CompilerParams(vmem_limit_bytes=4 * 1024 * 1024),
    )
    results = [put(*call(*(pltpu.with_memory_space_constraint(x, pltpu.HBM) for x in (start[0, 0, 0, p], stencils[:, 0, 0, 0])))) for p in range(probes)]
    basis = jnp.stack([r[0] for r in results])
    return basis[None, None, None], jnp.concatenate([r[1] for r in results])


def solution(mesh):
    sizes = tuple(mesh.shape[name] for name in ("gx", "gy", "gz"))
    return jax.shard_map(
        functools.partial(shards, sizes),
        mesh=mesh,
        in_specs=(P("gx", "gy", "gz", None, None, None), P(None, "gx", "gy", "gz", None, None)),
        out_specs=(P("gx", "gy", "gz", None, None, None, None), P()),
        check_vma=False,
    )
```

```python
import functools

import jax
import jax.numpy as jnp
from jax import lax
from jax.experimental import pallas as pl
from jax.experimental.pallas import tpu as pltpu
from jax.sharding import PartitionSpec as P

ITERS = 5
LANES = 128
SUB = 8
MESH = pl.DeviceIdType.MESH
KINDS = ("e", "x", "y", "z")
F32 = jnp.float32
BF16 = jnp.bfloat16
HIGHEST = lax.Precision.HIGHEST


def iota(shape, dim):
    return lax.broadcasted_iota(jnp.int32, shape, dim)


def split(x):
    hi = x.astype(BF16)
    return hi, (x - hi.astype(F32)).astype(BF16)


def exact(a, b):
    return lax.dot_general(a, b, (((1,), (0,)), ((), ())), precision=HIGHEST, preferred_element_type=F32)


def mul(a, b):
    return jnp.dot(a, b, preferred_element_type=F32)


def swap(x):
    sub = iota((1, SUB, LANES), 1) & 3
    apart = ((iota((1, SUB, LANES), 2) >> 5) - sub) & 3
    out = x
    for d in range(1, 4):
        far = pltpu.roll(x, 32 * d, 2)
        moved = jnp.where(sub < 4 - d, pltpu.roll(far, SUB - d, 1), pltpu.roll(far, 4 - d, 1))
        out = jnp.where(apart == d, moved, out)
    return out


def build_matrices(st, mx, my, mz, mzt, ya, yb):
    count = st.shape[1]
    wide = LANES
    spread = ((iota((wide, count), 0) & (count - 1)) == iota((wide, count), 1)).astype(F32)
    spread_t = ((iota((count, wide), 1) & (count - 1)) == iota((count, wide), 0)).astype(F32)
    same = (iota((wide, wide), 0) >> 5) == (iota((wide, wide), 1) >> 5)
    for slot, which in ((0, 5), (1, 2)):
        big = exact(exact(spread, st[which].T), spread_t)
        for ref, values in ((mz, jnp.where(same, big, 0.0)), (mzt, big)):
            hi, lo = split(values)
            ref[0:wide, slot * wide:(slot + 1) * wide] = hi
            ref[wide:2 * wide, slot * wide:(slot + 1) * wide] = hi
            ref[2 * wide:3 * wide, slot * wide:(slot + 1) * wide] = lo
    rows = 2 * count
    r = iota((rows, count), 0)
    pick = (((r >> 3) * 4 + (r & 3)) == iota((rows, count), 1)).astype(F32)
    cols = 3 * rows
    l = iota((count, cols), 1) & (rows - 1)
    pick_t = (((l >> 3) * 4 + (l & 3)) == iota((count, cols), 0)).astype(F32)
    same = ((iota((rows, cols), 0) >> 2) & 1) == ((iota((rows, cols), 1) >> 2) & 1)
    middle = (iota((rows, cols), 1) >= rows) & (iota((rows, cols), 1) < 2 * rows)
    for slot, which in ((0, 4), (1, 1)):
        big = jnp.where(same, exact(exact(pick, st[which]), pick_t), 0.0)
        hi = big.astype(BF16).astype(F32)
        my[slot * rows:(slot + 1) * rows, :] = jnp.where(middle, big - hi, hi).astype(BF16)
    cols = 7 * count
    row, col = iota((count, cols), 0), iota((count, cols), 1)
    block, extra, part = col >> 5, col >= 6 * count, (col >> 3) & 3
    source = jnp.where(extra, jnp.where((col & 2) == 0, 0, count - 1), col & (count - 1))
    tile = (source == row).astype(F32)
    big = jnp.where((extra & ((col & 4) == 0)) | (~extra & (block >= 3)), exact(st[3], tile), exact(st[0], tile))
    hi = big.astype(BF16).astype(F32)
    rest = (~extra & ((block == 1) | (block == 4))) | (extra & (part == 1))
    mx[...] = jnp.where(extra & (part == 3), 0.0, jnp.where(rest, big - hi, hi)).astype(BF16)
    r, b = iota((SUB, count), 0), iota((SUB, count), 1)
    ends = (b == jnp.where((r & 1) == 0, 0, count - 1)).astype(F32)
    area = ya.shape[1]
    widen = ((iota((count, area), 1) >> 5) == iota((count, area), 0)).astype(F32)
    mass = exact(exact(ends, st[4].T), widen)
    stiff = exact(exact(ends, st[1].T), widen)
    upper = iota((SUB, area), 0) < SUB // 2
    ya[...] = jnp.where(upper, stiff, mass)
    yb[...] = jnp.where(upper, mass, 0.0)


def through_z(u, rows_of, mz):
    nt = u(rows_of[0]).shape[1] // LANES
    blocks = [u(i) for i in rows_of]
    tiles = jnp.concatenate([block[:, LANES * t:LANES * (t + 1)] for block in blocks for t in range(nt)], axis=0)
    tiles = swap(tiles.reshape(-1, SUB, LANES)).reshape(-1, LANES)
    hi, lo = split(tiles)
    return mul(jnp.concatenate([hi, lo, hi], axis=1), mz)


def through_y(z, my):
    rows = my.shape[0] // 2
    packed = []
    for slot in range(2):
        part = z[:, slot * LANES:(slot + 1) * LANES]
        wide = jnp.concatenate([part[at:at + rows] for at in range(0, part.shape[0], rows)], axis=1)
        hi, lo = split(wide)
        packed.append(jnp.concatenate([hi, hi, lo], axis=0))
    both = mul(my, packed[0])
    return both[:rows], both[rows:] + mul(my[:rows], packed[1])


def swap_back(terms, t):
    width = terms[0].shape[1] // LANES
    stacked = jnp.stack([term[SUB * t:SUB * (t + 1), LANES * n:LANES * (n + 1)] for term in terms for n in range(width)])
    stacked = swap(stacked)
    return [[stacked[k * width + n] for n in range(width)] for k in range(2)]


def kernel(sizes, start_in, st_in, basis, coef, mx, my, mz, mzt, ya, yb, wt, field,
           zs, zr, xs, xz, xr, ys, yz, yr, es, ez, er, edge_slots, rows, hsend, hrecv, rsend, rrecv, ready, ws, start, st, loads):
    load_start = pltpu.make_async_copy(start_in, start, loads.at[0])
    load_st = pltpu.make_async_copy(st_in, st, loads.at[1])
    load_start.start()
    load_st.start()
    nx, ny, nz = sizes
    total = nx * ny * nz
    count, area = start.shape
    nt = area // LANES
    ni = count // SUB
    last = count - 1
    px, py, pz = lax.axis_index("gx"), lax.axis_index("gy"), lax.axis_index("gz")
    me = (px * ny + py) * nz + pz
    coords = (px, py, pz)
    there = [[coords[d] > 0, coords[d] < sizes[d] - 1] for d in range(3)]

    for ref in (zr, xr, yr, er):
        ref[...] = jnp.zeros_like(ref)
    barrier = pltpu.get_barrier_semaphore()

    def peer(k):
        p = lax.rem(me + k, total)
        return (p // (ny * nz), (p // nz) % ny, p % nz)

    def every_peer(act):
        if total > 64:
            def step(k, carry):
                act(peer(k))
                return carry

            lax.fori_loop(1, total, step, 0)
            return
        around = [[lax.rem(coords[d] + k, sizes[d]) if k else coords[d] for k in range(sizes[d])] for d in range(3)]
        for ky in range(ny - 1, -1, -1):
            for kx in range(nx - 1, -1, -1):
                for kz in range(nz):
                    if kx or ky or kz:
                        act((around[0][kx], around[1][ky], around[2][kz]))

    def neighbours(act):
        for dx in (-1, 0, 1):
            for dy in (-1, 0, 1):
                for dz in (-1, 0, 1):
                    if dx or dy or dz:
                        target = (px + dx, py + dy, pz + dz)
                        inside = None
                        for d, step in enumerate((dx, dy, dz)):
                            if step:
                                side = there[d][(step + 1) // 2]
                                inside = side if inside is None else inside & side

                        @pl.when(inside)
                        def _():
                            act(target)

    beside = [(coords[d] > 0).astype(jnp.int32) + (coords[d] < sizes[d] - 1).astype(jnp.int32) for d in range(3)]
    around_me = (1 + beside[0]) * (1 + beside[1]) * (1 + beside[2]) - 1
    amounts = {
        "e": lambda x, y, z: x * y * (1 + z),
        "x": lambda x, y, z: x * (1 + z),
        "y": lambda x, y, z: y * (1 + z),
        "z": lambda x, y, z: z,
    }
    sides = [(0,) if size == 1 else (1,) if size == 2 else (1, 2) for size in sizes]
    slots = {"e": edge_slots, "x": xr, "y": yr, "z": zr}

    rounds = max(sizes) - 2

    def call(r):
        neighbours(lambda target: pl.semaphore_signal(ready.at[r], inc=1, device_id=target, device_id_type=MESH))

    neighbours(lambda target: pl.semaphore_signal(barrier, inc=1, device_id=target, device_id_type=MESH))

    def shared(index, d):
        return ((index == 0) & there[d][0]) | ((index == last) & there[d][1])

    lane = iota((count, area), 1)
    ia, ib, ic = iota((count, area), 0), lane >> 5, lane & (count - 1)
    half = lambda index, d: jnp.where(shared(index, d), 0.5, 1.0)
    weight = half(ia, 0) * half(ib, 1) * half(ic, 2)
    wt[...] = weight.astype(F32)
    load_start.wait()
    field[...] = start[...] * wt[...]

    lane_c = iota((count, LANES), 1)
    face_c = (lane_c & (count - 1) == 0) | (lane_c & (count - 1) == last)
    even = (lane_c & 1) == 0
    lane8 = iota((SUB, LANES), 1)
    low8, high8 = lane8 < count, lane8 >= LANES - count
    lane1 = iota((1, LANES), 1)
    diag = iota((SUB, LANES), 0) == lane8

    def tile(t):
        return slice(t * LANES, (t + 1) * LANES)

    def halo_copies(phase):
        out = {name: [] for name in ("e", "ez", "x", "xz", "y", "yz", "z")}

        def add(name, src, into, *direction):
            there_all, target = None, {}
            for d, step in enumerate(direction):
                if step is not None:
                    there_all = there[d][step] if there_all is None else there_all & there[d][step]
            target = tuple(c if step is None else c + 2 * step - 1 for c, step in zip(coords, direction))
            copy = pltpu.make_async_remote_copy(
                src_ref=src, dst_ref=into, send_sem=hsend.at[KINDS.index(name[0])],
                recv_sem=hrecv.at[phase % 2, KINDS.index(name[0])], device_id=target, device_id_type=MESH)
            out[name].append((copy, there_all))

        for z in (None, 1, 0):
            back, kind = (0, "") if z is None else (2 - z, "z")
            for d in range(2):
                for e in range(2):
                    q = pl.ds(2 * d + e, 1)
                    src = es.at[phase, q] if z is None else ez.at[phase, z, q]
                    add("e" + kind, src, er.at[phase, back, pl.ds(2 * (1 - d) + 1 - e, 1)], d, e, z)
            for d in range(2):
                src = xs.at[phase, d] if z is None else xz.at[phase, z, d]
                add("x" + kind, src, xr.at[6 * phase + (1 - d) * 3 + back], d, None, z)
            for d in range(2):
                src = ys.at[phase, d] if z is None else yz.at[phase, z, d]
                add("y" + kind, src, yr.at[6 * phase + (1 - d) * 3 + back], None, d, z)
        for d in range(2):
            add("z", zs.at[phase], zr.at[2 * phase + 1 - d], None, None, d)
        return out

    def start_all(copies):
        for copy, exists, *_ in copies:
            @pl.when(exists)
            def _():
                copy.start()

    def across(value, z):
        c = iota(value.shape, 1) & (count - 1)
        if z == 1:
            return jnp.where(c == 0, pltpu.roll(value, LANES - last, 1), 0.0)
        return jnp.where(c == last, pltpu.roll(value, last, 1), 0.0)

    def send_halo(phase):
        copies = halo_copies(phase)

        def send(local, first):
            for t, value in local.items():
                field[:, tile(t)] = value
            for d in range(2):
                row = 0 if d == 0 else last
                for t, value in local.items():
                    xs[phase, d, t:t + 1, :] = value[row:row + 1]
                if first:
                    for e in range(2):
                        es[phase, 2 * d + e:2 * d + e + 1, :] = local[0 if e == 0 else nt - 1][row:row + 1]
            if first:
                start_all(copies["e"])
                for d in range(2):
                    packed = None
                    for i in range(ni):
                        block = local[0 if d == 0 else nt - 1][SUB * i:SUB * (i + 1)]
                        part = jnp.where(low8 if d == 0 else high8, block, 0.0)
                        shift = (count * i + d * count) % LANES
                        part = part if shift == 0 else pltpu.roll(part, shift, 1)
                        packed = part if packed is None else packed + part
                    ys[phase, d] = packed

        def rest():
            start_all(copies["x"])
            start_all(copies["y"])
            for z in range(2):
                ez[phase, z] = across(es[phase], z)
            start_all(copies["ez"])
            for z in range(2):
                for d in range(2):
                    xz[phase, z, d] = across(xs[phase, d], z)
            start_all(copies["xz"])
            for z in range(2):
                for d in range(2):
                    yz[phase, z, d] = across(ys[phase, d], z)
            start_all(copies["yz"])
            packed = None
            for t in range(nt):
                part = jnp.where(face_c, field[:, tile(t)], 0.0)
                part = part if t == 0 else pltpu.roll(part, 2 * t, 1)
                packed = part if packed is None else packed + part
            zs[phase] = packed
            start_all(copies["z"])

        return send, rest

    def take(kind, sem, phases):
        mine = amounts[kind](*beside)
        for amount in sorted({amounts[kind](x, y, z) for x in sides[0] for y in sides[1] for z in sides[2]}):
            if amount:
                @pl.when(mine == amount)
                def _():
                    into = slots[kind].at[pl.ds(0, amount * phases)]
                    pltpu.make_async_copy(into, into, sem).wait()

    def arrive(phase, kind):
        take(kind, hrecv.at[phase % 2, KINDS.index(kind)], 1)

    def sent(kind):
        take(kind, hsend.at[KINDS.index(kind)], ITERS + 1)

    def add_yz(phase):
        arrive(phase, "z")
        merged = jnp.where(even, pltpu.roll(zr[2 * phase], LANES - last, 1), pltpu.roll(zr[2 * phase + 1], last, 1))
        for t in range(nt):
            part = merged if t == 0 else pltpu.roll(merged, LANES - 2 * t, 1)
            field[:, tile(t)] += jnp.where(face_c, part, 0.0)
        arrive(phase, "y")
        for d in range(2):
            received = yr[6 * phase + 3 * d] + yr[6 * phase + 3 * d + 1] + yr[6 * phase + 3 * d + 2]
            for i in range(ni):
                shift = (-count * i - d * count) % LANES
                part = received if shift == 0 else pltpu.roll(received, shift, 1)
                field[SUB * i:SUB * (i + 1), tile(0 if d == 0 else nt - 1)] += jnp.where(low8 if d == 0 else high8, part, 0.0)

    def add_x(phase):
        arrive(phase, "x")
        for d in range(2):
            row = 0 if d == 0 else last
            received = xr[6 * phase + 3 * d] + xr[6 * phase + 3 * d + 1] + xr[6 * phase + 3 * d + 2]
            for t in range(nt):
                field[row:row + 1, tile(t)] += received[t:t + 1]

    def take_edges(phase, factor):
        arrive(phase, "e")
        out = er[phase, 0] + er[phase, 1] + er[phase, 2]
        side = (iota((SUB, LANES), 0) & 1) == 0
        out = jnp.where((side & high8) | (~side & low8), out, 0.0)
        return out if factor is None else out * factor

    def lines_of(edges):
        twice = edges + pltpu.roll(edges, SUB // 2, 0)
        twice = jnp.concatenate([twice, jnp.zeros_like(twice)], axis=0)
        hi, lo = split(twice)
        z = mul(jnp.concatenate([hi, lo, hi], axis=1), mzt[...])[:SUB]
        out = []
        for t in range(nt):
            line = ya[:, tile(t)] * z[:, :LANES] + yb[:, tile(t)] * z[:, LANES:]
            hi = line.astype(BF16).astype(F32)
            out.append(jnp.concatenate([hi, hi, line - hi, jnp.zeros_like(hi)], axis=0).astype(BF16))
        return out

    def add_edges(k, edges):
        for d in range(2):
            row = 0 if d == 0 else last
            ws[k, row:row + 1, tile(0)] += pltpu.roll(edges[2 * d:2 * d + 1], count, 1)
            ws[k, row:row + 1, tile(nt - 1)] += pltpu.roll(edges[2 * d + 1:2 * d + 2], LANES - count, 1)

    def send_dots(phase, products):
        packed = None
        for k, product in enumerate(products):
            acc = None
            for i in range(ni):
                for t in range(nt):
                    block = product[SUB * i:SUB * (i + 1), tile(t)]
                    acc = block if acc is None else acc + block
            line = jnp.where(iota((SUB, LANES), 0) == k, jnp.sum(acc, axis=0, keepdims=True), 0.0)
            packed = line if packed is None else packed + line
        sums = jnp.sum(packed, axis=1, keepdims=True)
        rows[phase, me] = jnp.sum(jnp.where(diag, sums, 0.0), axis=0, keepdims=True)

        def send(target):
            pltpu.make_async_remote_copy(
                src_ref=rows.at[phase, me], dst_ref=rows.at[phase, me], send_sem=rsend.at[phase],
                recv_sem=rrecv.at[phase], device_id=target, device_id_type=MESH).start()

        every_peer(send)

    def take_dots(phase):
        others = rows.at[phase, pl.ds(0, total - 1)]
        pltpu.make_async_copy(others, others, rrecv.at[phase]).wait()
        line = jnp.sum(rows[phase], axis=0)
        return jnp.sum(jnp.where(diag, line, 0.0), axis=1, keepdims=True)

    pl.semaphore_wait(barrier, around_me)
    send, rest = send_halo(0)
    value = field[...]
    send({t: value[:, tile(t)] for t in range(nt)}, True)
    rest()
    load_st.wait()
    build_matrices(st, mx, my, mz, mzt, ya, yb)
    for r in range(rounds):
        call(r)
        if r < rounds - 1:
            pl.semaphore_wait(ready.at[r], around_me)
    gram, rho = {}, [None]

    def gather(k):
        sums = take_dots(k)
        for i in range(k + 1):
            gram[i, k] = sums[i:i + 1]
        if k < ITERS:
            rho.append(sums[k + 1:k + 2] / sums[k:k + 1])

    factor = None

    def advance(k, inner):
        for i in range(ni):
            if (0 < i < ni - 1) == inner:
                part = slice(SUB * i, SUB * (i + 1))
                ws[k, part] = field[part] if k < 2 else field[part] * factor - ws[k - 1, part]

    middle, ends = list(range(1, ni - 1)), [0, ni - 1]
    block = lambda k: lambda i: ws[k, SUB * i:SUB * (i + 1)]
    for k in range(ITERS):
        add_yz(k)
        advance(k, True)
        inner = through_z(block(k), middle, mz[...])
        add_x(k)
        advance(k, False)
        outer = through_z(block(k), ends, mz[...])
        inner = through_y(inner, my[...])
        edges = take_edges(k, factor)
        lines = lines_of(edges)
        outer = through_y(outer, my[...])
        send, rest = send_halo(k + 1)
        order = [0, nt - 1] + list(range(1, nt - 1))
        for at in range(0, nt, 2):
            pieces = [[], []]
            for t in order[at:at + 2]:
                mid, end = swap_back(inner, t), swap_back(outer, t)
                for n in range(2):
                    pieces[n].append(jnp.concatenate([end[n][0]] + mid[n] + [end[n][1]], axis=0))
            stack = []
            for n in range(2):
                hi, lo = split(jnp.concatenate(pieces[n], axis=1))
                stack += [hi, hi, lo]
            stack.append(jnp.concatenate([lines[t] for t in order[at:at + 2]], axis=1))
            out = mul(mx[...], jnp.concatenate(stack, axis=0))
            send({t: out[:, LANES * n:LANES * (n + 1)] for n, t in enumerate(order[at:at + 2])}, at == 0)
        rest()
        if k == 0 and rounds > 0:
            pl.semaphore_wait(ready.at[rounds - 1], around_me)
        add_edges(k, edges)
        vector = ws[k]
        weighted = wt[...] * vector
        send_dots(k, [weighted * ws[i] for i in range(k + 1)] + [field[...] * vector])
        if k > 0:
            gather(k - 1)
            factor = 1.0 / rho[k]
    add_yz(ITERS)
    advance(ITERS, True)
    add_x(ITERS)
    advance(ITERS, False)
    add_edges(ITERS, take_edges(ITERS, factor))
    weighted = wt[...] * ws[ITERS]
    send_dots(ITERS, [weighted * ws[i] for i in range(ITERS + 1)])
    gather(ITERS - 1)

    upper, inverse, scale = {}, {}, []

    def column(k):
        for i in range(k):
            total_i = None
            for m in range(i + 1):
                term = inverse[m, i] * gram[m, k]
                total_i = term if total_i is None else total_i + term
            upper[i, k] = total_i
        rest = gram[k, k]
        for i in range(k):
            rest = rest - upper[i, k] * upper[i, k]
        upper[k, k] = jnp.sqrt(rest)
        inverse[k, k] = 1.0 / upper[k, k]
        for i in range(k):
            total_i = None
            for m in range(i, k):
                term = inverse[i, m] * upper[m, k]
                total_i = term if total_i is None else total_i + term
            inverse[i, k] = -total_i * inverse[k, k]
        if k > 0:
            out = ws[0] * inverse[0, k]
            for i in range(1, k + 1):
                out = out + ws[i] * inverse[i, k]
            basis[k - 1] = out

    for k in range(ITERS):
        column(k)
    for kind in KINDS:
        sent(kind)
    for phase in range(ITERS):
        others = rows.at[phase, pl.ds(0, total - 1)]
        pltpu.make_async_copy(others, others, rsend.at[phase]).wait()
    gather(ITERS)
    column(ITERS)
    row2, col2 = iota(coef.shape[1:], 0), iota(coef.shape[1:], 1)
    coefs = jnp.zeros(coef.shape[1:], F32)
    for k in range(ITERS):
        step = 1.0 if k == 0 else rho[k]
        alpha = step * (upper[k, k + 1] * inverse[k, k])
        if k > 0:
            alpha = alpha + rho[k]
            alpha = alpha - (1.0 if k == 1 else rho[k - 1]) * (upper[k - 1, k] * inverse[k - 1, k - 1])
        beta = step * (upper[k + 1, k + 1] * inverse[k, k])
        coefs = jnp.where((row2 == 0) & (col2 == k), alpha, coefs)
        coefs = jnp.where((row2 == 1) & (col2 == k), beta, coefs)
    coef[0] = coefs

    others = rows.at[ITERS, pl.ds(0, total - 1)]
    pltpu.make_async_copy(others, others, rsend.at[ITERS]).wait()


def store(basis, coef, basis_out, coef_out, sems):
    copies = [pltpu.make_async_copy(basis.at[i], basis_out.at[i], sems.at[i]) for i in range(ITERS)]
    copies.append(pltpu.make_async_copy(coef, coef_out, sems.at[ITERS]))
    for copy in copies:
        copy.start()
    for copy in copies:
        copy.wait()


def shards(sizes, start, stencils):
    probes, count, area = start.shape[3:]
    nt = area // LANES
    total = sizes[0] * sizes[1] * sizes[2]
    halos = ITERS + 1
    vmem = pl.BlockSpec(memory_space=pltpu.VMEM)
    call_shapes = (jax.ShapeDtypeStruct((ITERS, count, area), F32), jax.ShapeDtypeStruct((1, 2, ITERS), F32))
    call = pl.pallas_call(
        functools.partial(kernel, sizes),
        out_shape=call_shapes,
        in_specs=[pl.BlockSpec(memory_space=pltpu.HBM)] * 2,
        out_specs=(vmem, vmem),
        scratch_shapes=[
            pltpu.VMEM((count, 7 * count), BF16),
            pltpu.VMEM((4 * count, 6 * count), BF16),
            pltpu.VMEM((3 * LANES, 2 * LANES), BF16),
            pltpu.VMEM((3 * LANES, 2 * LANES), BF16),
            pltpu.VMEM((SUB, area), F32),
            pltpu.VMEM((SUB, area), F32),
            pltpu.VMEM((count, area), F32),
            pltpu.VMEM((count, area), F32),
            pltpu.VMEM((halos, count, LANES), F32),
            pltpu.VMEM((halos * 2, count, LANES), F32),
            pltpu.VMEM((halos, 2, nt, LANES), F32),
            pltpu.VMEM((halos, 2, 2, nt, LANES), F32),
            pltpu.VMEM((halos * 6, nt, LANES), F32),
            pltpu.VMEM((halos, 2, SUB, LANES), F32),
            pltpu.VMEM((halos, 2, 2, SUB, LANES), F32),
            pltpu.VMEM((halos * 6, SUB, LANES), F32),
            pltpu.VMEM((halos, 4, LANES), F32),
            pltpu.VMEM((halos, 2, 4, LANES), F32),
            pltpu.VMEM((halos, 3, SUB, LANES), F32),
            pltpu.VMEM((halos * 12, 1, LANES), F32),
            pltpu.VMEM((halos, total, 1, LANES), F32),
            pltpu.SemaphoreType.DMA((len(KINDS),)),
            pltpu.SemaphoreType.DMA((2, len(KINDS))),
            pltpu.SemaphoreType.DMA((halos,)),
            pltpu.SemaphoreType.DMA((halos,)),
            pltpu.SemaphoreType.REGULAR((max(1, max(sizes) - 2),)),
            pltpu.VMEM((halos, count, area), F32),
            pltpu.VMEM((count, area), F32),
            pltpu.VMEM(stencils.shape[:1] + stencils.shape[4:], F32),
            pltpu.SemaphoreType.DMA((2,)),
        ],
        compiler_params=pltpu.CompilerParams(collective_id=0, has_side_effects=True, vmem_limit_bytes=48 * 1024 * 1024),
    )
    hbm = pl.BlockSpec(memory_space=pltpu.HBM)
    put = pl.pallas_call(
        store,
        out_shape=call_shapes,
        in_specs=[vmem, vmem],
        out_specs=(hbm, hbm),
        scratch_shapes=[pltpu.SemaphoreType.DMA((ITERS + 1,))],
        compiler_params=pltpu.CompilerParams(vmem_limit_bytes=4 * 1024 * 1024),
    )
    results = [put(*call(*(pltpu.with_memory_space_constraint(x, pltpu.HBM) for x in (start[0, 0, 0, p], stencils[:, 0, 0, 0])))) for p in range(probes)]
    basis = jnp.stack([r[0] for r in results])
    return basis[None, None, None], jnp.concatenate([r[1] for r in results])


def solution(mesh):
    sizes = tuple(mesh.shape[name] for name in ("gx", "gy", "gz"))
    return jax.shard_map(
        functools.partial(shards, sizes),
        mesh=mesh,
        in_specs=(P("gx", "gy", "gz", None, None, None), P(None, "gx", "gy", "gz", None, None)),
        out_specs=(P("gx", "gy", "gz", None, None, None, None), P()),
        check_vma=False,
    )
```

```python
import functools

import jax
import jax.numpy as jnp
from jax import lax
from jax.experimental import pallas as pl
from jax.experimental.pallas import tpu as pltpu
from jax.sharding import PartitionSpec as P

ITERS = 5
LANES = 128
SUB = 8
MESH = pl.DeviceIdType.MESH
KINDS = ("e", "x", "y", "z")
F32 = jnp.float32
BF16 = jnp.bfloat16
HIGHEST = lax.Precision.HIGHEST


def iota(shape, dim):
    return lax.broadcasted_iota(jnp.int32, shape, dim)


def split(x):
    hi = x.astype(BF16)
    return hi, (x - hi.astype(F32)).astype(BF16)


def exact(a, b):
    return lax.dot_general(a, b, (((1,), (0,)), ((), ())), precision=HIGHEST, preferred_element_type=F32)


def mul(a, b):
    return jnp.dot(a, b, preferred_element_type=F32)


def swap(x):
    sub = iota((1, SUB, LANES), 1) & 3
    apart = ((iota((1, SUB, LANES), 2) >> 5) - sub) & 3
    out = x
    for d in range(1, 4):
        far = pltpu.roll(x, 32 * d, 2)
        moved = jnp.where(sub < 4 - d, pltpu.roll(far, SUB - d, 1), pltpu.roll(far, 4 - d, 1))
        out = jnp.where(apart == d, moved, out)
    return out


def build_matrices(st, mx, my, ym, mz, mzt, ya, yb):
    count = st.shape[1]
    wide = LANES
    spread = ((iota((wide, count), 0) & (count - 1)) == iota((wide, count), 1)).astype(F32)
    spread_t = ((iota((count, wide), 1) & (count - 1)) == iota((count, wide), 0)).astype(F32)
    same = (iota((wide, wide), 0) >> 5) == (iota((wide, wide), 1) >> 5)
    for slot, which in ((0, 5), (1, 2)):
        big = exact(exact(spread, st[which].T), spread_t)
        for ref, values in ((mz, jnp.where(same, big, 0.0)), (mzt, big)):
            hi, lo = split(values)
            ref[0:wide, slot * wide:(slot + 1) * wide] = hi
            ref[wide:2 * wide, slot * wide:(slot + 1) * wide] = hi
            ref[2 * wide:3 * wide, slot * wide:(slot + 1) * wide] = lo
    rows = 2 * count
    r = iota((rows, count), 0)
    place = r >> 3
    place = jnp.where(place == 0, 0, jnp.where(place == 1, rows // SUB - 1, place - 1))
    pick = ((place * 4 + (r & 3)) == iota((rows, count), 1)).astype(F32)
    cols = 3 * rows
    l = iota((count, cols), 1) & (rows - 1)
    pick_t = (((l >> 3) * 4 + (l & 3)) == iota((count, cols), 0)).astype(F32)
    same = ((iota((rows, cols), 0) >> 2) & 1) == ((iota((rows, cols), 1) >> 2) & 1)
    middle = (iota((rows, cols), 1) >= rows) & (iota((rows, cols), 1) < 2 * rows)
    for slot, which in ((0, 4), (1, 1)):
        big = jnp.where(same, exact(exact(pick, st[which]), pick_t), 0.0)
        hi = big.astype(BF16).astype(F32)
        big = jnp.where(middle, big - hi, hi).astype(BF16)
        if slot == 0:
            ym[...] = big
        for at in range(0, rows, 2 * SUB):
            my[2 * at + 2 * SUB * slot:2 * at + 2 * SUB * (slot + 1), :] = big[at:at + 2 * SUB]
    cols = 7 * count
    row, col = iota((count, cols), 0), iota((count, cols), 1)
    extra, part = col >= 6 * count, (col >> 3) & 3
    wide, within = 2 * SUB, col & (2 * SUB - 1)
    outer = (col >= 6 * wide) & ~extra
    block = jnp.where(outer, (col >> 4) - 6, col >> 4)
    source = jnp.where(outer, jnp.where(within < SUB, within, count - wide + within), SUB + within)
    source = jnp.where(extra, jnp.where((col & 2) == 0, 0, count - 1), source)
    tile = (source == row).astype(F32)
    big = jnp.where((extra & ((col & 4) == 0)) | (~extra & (block >= 3)), exact(st[3], tile), exact(st[0], tile))
    hi = big.astype(BF16).astype(F32)
    rest = (~extra & ((block == 1) | (block == 4))) | (extra & (part == 1))
    mx[...] = jnp.where(extra & (part == 3), 0.0, jnp.where(rest, big - hi, hi)).astype(BF16)
    r, b = iota((SUB, count), 0), iota((SUB, count), 1)
    ends = (b == jnp.where((r & 1) == 0, 0, count - 1)).astype(F32)
    area = ya.shape[1]
    widen = ((iota((count, area), 1) >> 5) == iota((count, area), 0)).astype(F32)
    mass = exact(exact(ends, st[4].T), widen)
    stiff = exact(exact(ends, st[1].T), widen)
    upper = iota((SUB, area), 0) < SUB // 2
    ya[...] = jnp.where(upper, stiff, mass)
    yb[...] = jnp.where(upper, mass, 0.0)


def through_z(u, rows_of, mz):
    nt = u(rows_of[0]).shape[1] // LANES
    blocks = [u(i) for i in rows_of]
    tiles = jnp.concatenate([block[:, LANES * t:LANES * (t + 1)] for block in blocks for t in range(nt)], axis=0)
    tiles = swap(tiles.reshape(-1, SUB, LANES)).reshape(-1, LANES)
    hi, lo = split(tiles)
    return mul(jnp.concatenate([hi, lo, hi], axis=1), mz)


def through_y(z, my, ym):
    rows = ym.shape[0]
    packed = []
    for slot in range(2):
        part = z[:, slot * LANES:(slot + 1) * LANES]
        wide = jnp.concatenate([part[at:at + rows] for at in range(0, part.shape[0], rows)], axis=1)
        hi, lo = split(wide)
        packed.append(jnp.concatenate([hi, hi, lo], axis=0))
    second = mul(ym, packed[1])
    both = mul(my, packed[0])
    pairs = []
    for at in range(0, rows, 2 * SUB):
        pairs.append((both[2 * at:2 * at + 2 * SUB], both[2 * at + 2 * SUB:2 * at + 4 * SUB] + second[at:at + 2 * SUB]))
    return pairs


def swap_back(terms, n):
    width = terms[0].shape[1] // LANES
    stacked = jnp.stack([term[SUB * n:SUB * (n + 1), LANES * i:LANES * (i + 1)] for term in terms for i in range(width)])
    stacked = swap(stacked)
    return [[stacked[k * width + i] for i in range(width)] for k in range(2)]


def kernel(sizes, start_in, st_in, basis, coef, mx, my, ym, mz, mzt, ya, yb, wt, field,
           zs, zr, xs, xz, xr, ys, yz, yr, es, ez, er, edge_slots, rows, hsend, hrecv, rsend, rrecv, ready, ws, start, st, loads, mid):
    nx, ny, nz = sizes
    total = nx * ny * nz
    count, area = start.shape
    nt = area // LANES
    ni = count // SUB
    last = count - 1
    px, py, pz = lax.axis_index("gx"), lax.axis_index("gy"), lax.axis_index("gz")
    me = (px * ny + py) * nz + pz
    coords = (px, py, pz)
    there = [[coords[d] > 0, coords[d] < sizes[d] - 1] for d in range(3)]

    load_start = pltpu.make_async_copy(start_in, start, loads.at[0])
    load_st = pltpu.make_async_copy(st_in, st, loads.at[1])
    load_start.start()
    load_st.start()
    barrier = pltpu.get_barrier_semaphore()

    def peer(k):
        p = lax.rem(me + k, total)
        return (p // (ny * nz), (p // nz) % ny, p % nz)

    def every_peer(act):
        if total > 64:
            def step(k, carry):
                act(peer(k))
                return carry

            lax.fori_loop(1, total, step, 0)
            return
        step = lambda d, k: coords[d] ^ k if sizes[d] & (sizes[d] - 1) == 0 else lax.rem(coords[d] + k, sizes[d])
        around = [[step(d, k) if k else coords[d] for k in range(sizes[d])] for d in range(3)]
        for ky in range(ny - 1, -1, -1):
            for kx in range(nx - 1, -1, -1):
                for kz in range(nz):
                    if kx or ky or kz:
                        act((around[0][kx], around[1][ky], around[2][kz]))

    def neighbours(act):
        around = [(dx, dy, dz) for dx in (-1, 0, 1) for dy in (-1, 0, 1) for dz in (0, -1, 1) if dx or dy or dz]
        for dx, dy, dz in sorted(around, key=lambda step: -2 * abs(step[0]) - abs(step[1])):
            target = (px + dx, py + dy, pz + dz)
            inside = None
            for d, step in enumerate((dx, dy, dz)):
                if step:
                    side = there[d][(step + 1) // 2]
                    inside = side if inside is None else inside & side

            @pl.when(inside)
            def _():
                act(target)

    beside = [(coords[d] > 0).astype(jnp.int32) + (coords[d] < sizes[d] - 1).astype(jnp.int32) for d in range(3)]
    around_me = (1 + beside[0]) * (1 + beside[1]) * (1 + beside[2]) - 1
    amounts = {
        "e": lambda x, y, z: x * y * (1 + z),
        "x": lambda x, y, z: x * (1 + z),
        "y": lambda x, y, z: y * (1 + z),
        "z": lambda x, y, z: z,
    }
    sides = [(0,) if size == 1 else (1,) if size == 2 else (1, 2) for size in sizes]
    slots = {"e": edge_slots, "x": xr, "y": yr, "z": zr}

    rounds = max(sizes) - 2

    def call(r):
        neighbours(lambda target: pl.semaphore_signal(ready.at[r], inc=1, device_id=target, device_id_type=MESH))

    neighbours(lambda target: pl.semaphore_signal(barrier, inc=1, device_id=target, device_id_type=MESH))

    def clear(missing, refs):
        @pl.when(missing)
        def _():
            for ref in refs:
                ref[...] = jnp.zeros_like(ref)

    phases = range(ITERS + 1)
    for phase in phases:
        er[phase, :, SUB // 2:, :] = jnp.zeros((3, SUB // 2, LANES), F32)
    for d in range(2):
        clear(~there[2][d], [zr.at[2 * phase + d] for phase in phases])
        clear(~there[0][d], [xr.at[pl.ds(6 * phase + 3 * d, 3)] for phase in phases])
        clear(~there[1][d], [yr.at[pl.ds(6 * phase + 3 * d, 3)] for phase in phases])
        for z in range(2):
            clear(there[0][d] & ~there[2][z], [xr.at[6 * phase + 3 * d + 1 + z] for phase in phases])
            clear(there[1][d] & ~there[2][z], [yr.at[6 * phase + 3 * d + 1 + z] for phase in phases])
        for e in range(2):
            q = pl.ds(2 * d + e, 1)
            both = there[0][d] & there[1][e]
            clear(~both, [er.at[phase, :, q] for phase in phases])
            for z in range(2):
                clear(both & ~there[2][z], [er.at[phase, 1 + z, q] for phase in phases])

    def shared(index, d):
        return ((index == 0) & there[d][0]) | ((index == last) & there[d][1])

    lane = iota((count, area), 1)
    ia, ib, ic = iota((count, area), 0), lane >> 5, lane & (count - 1)
    half = lambda index, d: jnp.where(shared(index, d), 0.5, 1.0)
    weight = half(ia, 0) * half(ib, 1) * half(ic, 2)
    wt[...] = weight.astype(F32)
    load_start.wait()
    field[...] = start[...] * wt[...]

    lane_c = iota((count, LANES), 1)
    face_c = (lane_c & (count - 1) == 0) | (lane_c & (count - 1) == last)
    even = (lane_c & 1) == 0
    lane8 = iota((SUB, LANES), 1)
    low8, high8 = lane8 < count, lane8 >= LANES - count
    lane1 = iota((1, LANES), 1)
    diag = iota((SUB, LANES), 0) == lane8

    def tile(t):
        return slice(t * LANES, (t + 1) * LANES)

    def halo_copies(phase):
        out = {name: [] for name in ("e", "ez", "x", "xz", "y", "yz", "z")}

        def add(name, src, into, *direction):
            there_all, target = None, {}
            for d, step in enumerate(direction):
                if step is not None:
                    there_all = there[d][step] if there_all is None else there_all & there[d][step]
            target = tuple(c if step is None else c + 2 * step - 1 for c, step in zip(coords, direction))
            copy = pltpu.make_async_remote_copy(
                src_ref=src, dst_ref=into, send_sem=hsend.at[KINDS.index(name[0])],
                recv_sem=hrecv.at[phase % 2, KINDS.index(name[0])], device_id=target, device_id_type=MESH)
            out[name].append((copy, there_all))

        for z in (None, 1, 0):
            back, kind = (0, "") if z is None else (2 - z, "z")
            for d in range(2):
                for e in range(2):
                    q = pl.ds(2 * d + e, 1)
                    src = es.at[phase, q] if z is None else ez.at[phase, z, q]
                    add("e" + kind, src, er.at[phase, back, pl.ds(2 * (1 - d) + 1 - e, 1)], d, e, z)
            for d in range(2):
                src = xs.at[phase, d] if z is None else xz.at[phase, z, d]
                add("x" + kind, src, xr.at[6 * phase + (1 - d) * 3 + back], d, None, z)
            for d in range(2):
                src = ys.at[phase, d] if z is None else yz.at[phase, z, d]
                add("y" + kind, src, yr.at[6 * phase + (1 - d) * 3 + back], None, d, z)
        for d in range(2):
            add("z", zs.at[phase], zr.at[2 * phase + 1 - d], None, None, d)
        return out

    def start_all(copies):
        for copy, exists, *_ in copies:
            @pl.when(exists)
            def _():
                copy.start()

    def across(value, z):
        c = iota(value.shape, 1) & (count - 1)
        if z == 1:
            return jnp.where(c == 0, pltpu.roll(value, LANES - last, 1), 0.0)
        return jnp.where(c == last, pltpu.roll(value, last, 1), 0.0)

    def send_halo(phase):
        copies = halo_copies(phase)

        def send(local, first):
            for t, value in local.items():
                field[:, tile(t)] = value
            for d in range(2):
                row = 0 if d == 0 else last
                for t, value in local.items():
                    xs[phase, d, t:t + 1, :] = value[row:row + 1]
                if first:
                    for e in range(2):
                        es[phase, 2 * d + e:2 * d + e + 1, :] = local[0 if e == 0 else nt - 1][row:row + 1]
            if first:
                for d in range(2):
                    packed = None
                    for i in range(ni):
                        block = local[0 if d == 0 else nt - 1][SUB * i:SUB * (i + 1)]
                        part = jnp.where(low8 if d == 0 else high8, block, 0.0)
                        shift = (count * i + d * count) % LANES
                        part = part if shift == 0 else pltpu.roll(part, shift, 1)
                        packed = part if packed is None else packed + part
                    ys[phase, d] = packed

        def rest():
            start_all(copies["x"])
            start_all(copies["e"])
            start_all(copies["y"])
            for z in range(2):
                ez[phase, z] = across(es[phase], z)
            start_all(copies["ez"])
            for z in range(2):
                for d in range(2):
                    xz[phase, z, d] = across(xs[phase, d], z)
            start_all(copies["xz"])
            for z in range(2):
                for d in range(2):
                    yz[phase, z, d] = across(ys[phase, d], z)
            start_all(copies["yz"])
            packed = None
            for t in range(nt):
                part = jnp.where(face_c, field[:, tile(t)], 0.0)
                part = part if t == 0 else pltpu.roll(part, 2 * t, 1)
                packed = part if packed is None else packed + part
            zs[phase] = packed
            start_all(copies["z"])

        return send, rest

    def take(kind, sem, phases):
        mine = amounts[kind](*beside)
        for amount in sorted({amounts[kind](x, y, z) for x in sides[0] for y in sides[1] for z in sides[2]}):
            if amount:
                @pl.when(mine == amount)
                def _():
                    into = slots[kind].at[pl.ds(0, amount * phases)]
                    pltpu.make_async_copy(into, into, sem).wait()

    def arrive(phase, kind):
        take(kind, hrecv.at[phase % 2, KINDS.index(kind)], 1)

    def sent(kind):
        take(kind, hsend.at[KINDS.index(kind)], ITERS + 1)

    def add_yz(phase):
        arrive(phase, "z")
        merged = jnp.where(even, pltpu.roll(zr[2 * phase], LANES - last, 1), pltpu.roll(zr[2 * phase + 1], last, 1))
        for t in range(nt):
            part = merged if t == 0 else pltpu.roll(merged, LANES - 2 * t, 1)
            field[:, tile(t)] += jnp.where(face_c, part, 0.0)
        arrive(phase, "y")
        for d in range(2):
            received = yr[6 * phase + 3 * d] + yr[6 * phase + 3 * d + 1] + yr[6 * phase + 3 * d + 2]
            for i in range(ni):
                shift = (-count * i - d * count) % LANES
                part = received if shift == 0 else pltpu.roll(received, shift, 1)
                field[SUB * i:SUB * (i + 1), tile(0 if d == 0 else nt - 1)] += jnp.where(low8 if d == 0 else high8, part, 0.0)

    def add_x(phase):
        arrive(phase, "x")
        for d in range(2):
            row = 0 if d == 0 else last
            received = xr[6 * phase + 3 * d] + xr[6 * phase + 3 * d + 1] + xr[6 * phase + 3 * d + 2]
            for t in range(nt):
                field[row:row + 1, tile(t)] += received[t:t + 1]

    def take_edges(phase, factor):
        arrive(phase, "e")
        out = er[phase, 0] + er[phase, 1] + er[phase, 2]
        side = (iota((SUB, LANES), 0) & 1) == 0
        out = jnp.where((side & high8) | (~side & low8), out, 0.0)
        return out if factor is None else out * factor

    def lines_of(edges):
        twice = edges + pltpu.roll(edges, SUB // 2, 0)
        twice = jnp.concatenate([twice, jnp.zeros_like(twice)], axis=0)
        hi, lo = split(twice)
        z = mul(jnp.concatenate([hi, lo, hi], axis=1), mzt[...])[:SUB]
        out = []
        for t in range(nt):
            line = ya[:, tile(t)] * z[:, :LANES] + yb[:, tile(t)] * z[:, LANES:]
            hi = line.astype(BF16).astype(F32)
            out.append(jnp.concatenate([hi, hi, line - hi, jnp.zeros_like(hi)], axis=0).astype(BF16))
        return out

    def add_edges(k, edges):
        for d in range(2):
            row = 0 if d == 0 else last
            ws[k, row:row + 1, tile(0)] += pltpu.roll(edges[2 * d:2 * d + 1], count, 1)
            ws[k, row:row + 1, tile(nt - 1)] += pltpu.roll(edges[2 * d + 1:2 * d + 2], LANES - count, 1)

    def send_dots(phase, products):
        packed = None
        for k, product in enumerate(products):
            acc = None
            for i in range(ni):
                for t in range(nt):
                    block = product[SUB * i:SUB * (i + 1), tile(t)]
                    acc = block if acc is None else acc + block
            line = jnp.where(iota((SUB, LANES), 0) == k, jnp.sum(acc, axis=0, keepdims=True), 0.0)
            packed = line if packed is None else packed + line
        sums = jnp.sum(packed, axis=1, keepdims=True)
        rows[phase, me] = jnp.sum(jnp.where(diag, sums, 0.0), axis=0, keepdims=True)

        def send(target):
            pltpu.make_async_remote_copy(
                src_ref=rows.at[phase, me], dst_ref=rows.at[phase, me], send_sem=rsend.at[phase],
                recv_sem=rrecv.at[phase], device_id=target, device_id_type=MESH).start()

        every_peer(send)

    def take_dots(phase):
        others = rows.at[phase, pl.ds(0, total - 1)]
        pltpu.make_async_copy(others, others, rrecv.at[phase]).wait()
        line = jnp.sum(rows[phase], axis=0)
        return jnp.sum(jnp.where(diag, line, 0.0), axis=1, keepdims=True)

    pl.semaphore_wait(barrier, around_me)
    send, rest = send_halo(0)
    value = field[...]
    send({t: value[:, tile(t)] for t in range(nt)}, True)
    rest()
    load_st.wait()
    build_matrices(st, mx, my, ym, mz, mzt, ya, yb)
    for r in range(rounds):
        call(r)
        if r < rounds - 1:
            pl.semaphore_wait(ready.at[r], around_me)
    gram, rho = {}, [None]

    def gather(k):
        sums = take_dots(k)
        for i in range(k + 1):
            gram[i, k] = sums[i:i + 1]
        if k < ITERS:
            rho.append(sums[k + 1:k + 2] / sums[k:k + 1])

    factor = None

    def advance(k, inner):
        for i in range(ni):
            if (0 < i < ni - 1) == inner:
                part = slice(SUB * i, SUB * (i + 1))
                ws[k, part] = field[part] if k < 2 else field[part] * factor - ws[k - 1, part]

    middle, ends = list(range(1, ni - 1)), [0, ni - 1]
    block = lambda k: lambda i: ws[k, SUB * i:SUB * (i + 1)]
    for k in range(ITERS):
        add_yz(k)
        advance(k, True)
        inner = through_z(block(k), middle, mz[...])
        add_x(k)
        advance(k, False)
        outer = through_z(block(k), ends, mz[...])
        inner = through_y(inner, my[...], ym[...])
        edges = take_edges(k, factor)
        for p in range(nt // 2):
            swapped = [swap_back(inner[p], n) for n in range(2)]
            for j in range(2):
                hi, lo = split(jnp.concatenate([jnp.concatenate(part[j], axis=0) for part in swapped], axis=1))
                mid[p, 2 * j] = hi
                mid[p, 2 * j + 1] = lo
        outer = through_y(outer, my[...], ym[...])
        lines = lines_of(edges)
        send, rest = send_halo(k + 1)
        order = [0, nt - 1] + list(range(1, nt - 1))
        for p in range(nt // 2):
            pair = order[2 * p:2 * p + 2]
            stack = []
            for j in range(2):
                stack += [mid[p, 2 * j], mid[p, 2 * j], mid[p, 2 * j + 1]]
            swapped = [swap_back(outer[p], n) for n in range(2)]
            for j in range(2):
                hi, lo = split(jnp.concatenate([jnp.concatenate(part[j], axis=0) for part in swapped], axis=1))
                stack += [hi, hi, lo]
            stack.append(jnp.concatenate([lines[t] for t in pair], axis=1))
            out = mul(mx[...], jnp.concatenate(stack, axis=0))
            send({t: out[:, LANES * n:LANES * (n + 1)] for n, t in enumerate(pair)}, p == 0)
        rest()
        if k == 0 and rounds > 0:
            pl.semaphore_wait(ready.at[rounds - 1], around_me)
        add_edges(k, edges)
        vector = ws[k]
        weighted = wt[...] * vector
        send_dots(k, [weighted * ws[i] for i in range(k + 1)] + [field[...] * vector])
        if k > 0:
            gather(k - 1)
            factor = 1.0 / rho[k]
    add_yz(ITERS)
    advance(ITERS, True)
    add_x(ITERS)
    advance(ITERS, False)
    add_edges(ITERS, take_edges(ITERS, factor))
    weighted = wt[...] * ws[ITERS]
    send_dots(ITERS, [weighted * ws[i] for i in range(ITERS + 1)])
    gather(ITERS - 1)

    upper, inverse, scale = {}, {}, []

    def column(k):
        for i in range(k):
            total_i = None
            for m in range(i + 1):
                term = inverse[m, i] * gram[m, k]
                total_i = term if total_i is None else total_i + term
            upper[i, k] = total_i
        rest = gram[k, k]
        for i in range(k):
            rest = rest - upper[i, k] * upper[i, k]
        upper[k, k] = jnp.sqrt(rest)
        inverse[k, k] = 1.0 / upper[k, k]
        for i in range(k):
            total_i = None
            for m in range(i, k):
                term = inverse[i, m] * upper[m, k]
                total_i = term if total_i is None else total_i + term
            inverse[i, k] = -total_i * inverse[k, k]
        if k > 0:
            out = ws[0] * inverse[0, k]
            for i in range(1, k + 1):
                out = out + ws[i] * inverse[i, k]
            basis[k - 1] = out

    for k in range(ITERS):
        column(k)
    for kind in KINDS:
        sent(kind)
    for phase in range(ITERS):
        others = rows.at[phase, pl.ds(0, total - 1)]
        pltpu.make_async_copy(others, others, rsend.at[phase]).wait()
    gather(ITERS)
    column(ITERS)
    row2, col2 = iota(coef.shape[1:], 0), iota(coef.shape[1:], 1)
    coefs = jnp.zeros(coef.shape[1:], F32)
    for k in range(ITERS):
        step = 1.0 if k == 0 else rho[k]
        alpha = step * (upper[k, k + 1] * inverse[k, k])
        if k > 0:
            alpha = alpha + rho[k]
            alpha = alpha - (1.0 if k == 1 else rho[k - 1]) * (upper[k - 1, k] * inverse[k - 1, k - 1])
        beta = step * (upper[k + 1, k + 1] * inverse[k, k])
        coefs = jnp.where((row2 == 0) & (col2 == k), alpha, coefs)
        coefs = jnp.where((row2 == 1) & (col2 == k), beta, coefs)
    coef[0] = coefs

    others = rows.at[ITERS, pl.ds(0, total - 1)]
    pltpu.make_async_copy(others, others, rsend.at[ITERS]).wait()


def store(basis, coef, basis_out, coef_out, sems):
    copies = [pltpu.make_async_copy(basis.at[i], basis_out.at[i], sems.at[i]) for i in range(ITERS)]
    copies.append(pltpu.make_async_copy(coef, coef_out, sems.at[ITERS]))
    for copy in copies:
        copy.start()
    for copy in copies:
        copy.wait()


def shards(sizes, start, stencils):
    probes, count, area = start.shape[3:]
    nt = area // LANES
    total = sizes[0] * sizes[1] * sizes[2]
    halos = ITERS + 1
    vmem = pl.BlockSpec(memory_space=pltpu.VMEM)
    call_shapes = (jax.ShapeDtypeStruct((ITERS, count, area), F32), jax.ShapeDtypeStruct((1, 2, ITERS), F32))
    call = pl.pallas_call(
        functools.partial(kernel, sizes),
        out_shape=call_shapes,
        in_specs=[pl.BlockSpec(memory_space=pltpu.HBM)] * 2,
        out_specs=(vmem, vmem),
        scratch_shapes=[
            pltpu.VMEM((count, 7 * count), BF16),
            pltpu.VMEM((4 * count, 6 * count), BF16),
            pltpu.VMEM((2 * count, 6 * count), BF16),
            pltpu.VMEM((3 * LANES, 2 * LANES), BF16),
            pltpu.VMEM((3 * LANES, 2 * LANES), BF16),
            pltpu.VMEM((SUB, area), F32),
            pltpu.VMEM((SUB, area), F32),
            pltpu.VMEM((count, area), F32),
            pltpu.VMEM((count, area), F32),
            pltpu.VMEM((halos, count, LANES), F32),
            pltpu.VMEM((halos * 2, count, LANES), F32),
            pltpu.VMEM((halos, 2, nt, LANES), F32),
            pltpu.VMEM((halos, 2, 2, nt, LANES), F32),
            pltpu.VMEM((halos * 6, nt, LANES), F32),
            pltpu.VMEM((halos, 2, SUB, LANES), F32),
            pltpu.VMEM((halos, 2, 2, SUB, LANES), F32),
            pltpu.VMEM((halos * 6, SUB, LANES), F32),
            pltpu.VMEM((halos, 4, LANES), F32),
            pltpu.VMEM((halos, 2, 4, LANES), F32),
            pltpu.VMEM((halos, 3, SUB, LANES), F32),
            pltpu.VMEM((halos * 12, 1, LANES), F32),
            pltpu.VMEM((halos, total, 1, LANES), F32),
            pltpu.SemaphoreType.DMA((len(KINDS),)),
            pltpu.SemaphoreType.DMA((2, len(KINDS))),
            pltpu.SemaphoreType.DMA((halos,)),
            pltpu.SemaphoreType.DMA((halos,)),
            pltpu.SemaphoreType.REGULAR((max(1, max(sizes) - 2),)),
            pltpu.VMEM((halos, count, area), F32),
            pltpu.VMEM((count, area), F32),
            pltpu.VMEM(stencils.shape[:1] + stencils.shape[4:], F32),
            pltpu.SemaphoreType.DMA((2,)),
            pltpu.VMEM((nt // 2, 4, 2 * SUB, 2 * LANES), BF16),
        ],
        compiler_params=pltpu.CompilerParams(collective_id=0, has_side_effects=True, vmem_limit_bytes=48 * 1024 * 1024),
    )
    hbm = pl.BlockSpec(memory_space=pltpu.HBM)
    put = pl.pallas_call(
        store,
        out_shape=call_shapes,
        in_specs=[vmem, vmem],
        out_specs=(hbm, hbm),
        scratch_shapes=[pltpu.SemaphoreType.DMA((ITERS + 1,))],
        compiler_params=pltpu.CompilerParams(vmem_limit_bytes=4 * 1024 * 1024),
    )
    results = [put(*call(*(pltpu.with_memory_space_constraint(x, pltpu.HBM) for x in (start[0, 0, 0, p], stencils[:, 0, 0, 0])))) for p in range(probes)]
    basis = jnp.stack([r[0] for r in results])
    return basis[None, None, None], jnp.concatenate([r[1] for r in results])


def solution(mesh):
    sizes = tuple(mesh.shape[name] for name in ("gx", "gy", "gz"))
    return jax.shard_map(
        functools.partial(shards, sizes),
        mesh=mesh,
        in_specs=(P("gx", "gy", "gz", None, None, None), P(None, "gx", "gy", "gz", None, None)),
        out_specs=(P("gx", "gy", "gz", None, None, None, None), P()),
        check_vma=False,
    )
```

```python
import functools

import jax
import jax.numpy as jnp
from jax import lax
from jax.experimental import pallas as pl
from jax.experimental.pallas import tpu as pltpu
from jax.sharding import PartitionSpec as P

ITERS = 5
LANES = 128
SUB = 8
MESH = pl.DeviceIdType.MESH
KINDS = ("e", "x", "y", "z")
F32 = jnp.float32
BF16 = jnp.bfloat16
HIGHEST = lax.Precision.HIGHEST


def iota(shape, dim):
    return lax.broadcasted_iota(jnp.int32, shape, dim)


def split(x):
    hi = x.astype(BF16)
    return hi, (x - hi.astype(F32)).astype(BF16)


def exact(a, b):
    return lax.dot_general(a, b, (((1,), (0,)), ((), ())), precision=HIGHEST, preferred_element_type=F32)


def mul(a, b):
    return jnp.dot(a, b, preferred_element_type=F32)


def swap(x):
    sub = iota((1, SUB, LANES), 1) & 3
    apart = ((iota((1, SUB, LANES), 2) >> 5) - sub) & 3
    out = x
    for d in range(1, 4):
        far = pltpu.roll(x, 32 * d, 2)
        moved = jnp.where(sub < 4 - d, pltpu.roll(far, SUB - d, 1), pltpu.roll(far, 4 - d, 1))
        out = jnp.where(apart == d, moved, out)
    return out


def build_matrices(st, mx, my, ym, mz, mzt, ya, yb):
    count = st.shape[1]
    wide = LANES
    spread = ((iota((wide, count), 0) & (count - 1)) == iota((wide, count), 1)).astype(F32)
    spread_t = ((iota((count, wide), 1) & (count - 1)) == iota((count, wide), 0)).astype(F32)
    same = (iota((wide, wide), 0) >> 5) == (iota((wide, wide), 1) >> 5)
    for slot, which in ((0, 5), (1, 2)):
        big = exact(exact(spread, st[which].T), spread_t)
        for ref, values in ((mz, jnp.where(same, big, 0.0)), (mzt, big)):
            hi, lo = split(values)
            ref[0:wide, slot * wide:(slot + 1) * wide] = hi
            ref[wide:2 * wide, slot * wide:(slot + 1) * wide] = hi
            ref[2 * wide:3 * wide, slot * wide:(slot + 1) * wide] = lo
    rows = 2 * count
    r = iota((rows, count), 0)
    place = r >> 3
    place = jnp.where(place == 0, 0, jnp.where(place == 1, rows // SUB - 1, place - 1))
    pick = ((place * 4 + (r & 3)) == iota((rows, count), 1)).astype(F32)
    cols = 3 * rows
    l = iota((count, cols), 1) & (rows - 1)
    pick_t = (((l >> 3) * 4 + (l & 3)) == iota((count, cols), 0)).astype(F32)
    same = ((iota((rows, cols), 0) >> 2) & 1) == ((iota((rows, cols), 1) >> 2) & 1)
    middle = (iota((rows, cols), 1) >= rows) & (iota((rows, cols), 1) < 2 * rows)
    for slot, which in ((0, 4), (1, 1)):
        big = jnp.where(same, exact(exact(pick, st[which]), pick_t), 0.0)
        hi = big.astype(BF16).astype(F32)
        big = jnp.where(middle, big - hi, hi).astype(BF16)
        if slot == 0:
            ym[...] = big
        for at in range(0, rows, 2 * SUB):
            my[2 * at + 2 * SUB * slot:2 * at + 2 * SUB * (slot + 1), :] = big[at:at + 2 * SUB]
    cols = 7 * count
    row, col = iota((count, cols), 0), iota((count, cols), 1)
    extra, part = col >= 6 * count, (col >> 3) & 3
    wide, within = 2 * SUB, col & (2 * SUB - 1)
    outer = (col >= 6 * wide) & ~extra
    block = jnp.where(outer, (col >> 4) - 6, col >> 4)
    source = jnp.where(outer, jnp.where(within < SUB, within, count - wide + within), SUB + within)
    source = jnp.where(extra, jnp.where((col & 2) == 0, 0, count - 1), source)
    tile = (source == row).astype(F32)
    big = jnp.where((extra & ((col & 4) == 0)) | (~extra & (block >= 3)), exact(st[3], tile), exact(st[0], tile))
    hi = big.astype(BF16).astype(F32)
    rest = (~extra & ((block == 1) | (block == 4))) | (extra & (part == 1))
    mx[...] = jnp.where(extra & (part == 3), 0.0, jnp.where(rest, big - hi, hi)).astype(BF16)
    r, b = iota((SUB, count), 0), iota((SUB, count), 1)
    ends = (b == jnp.where((r & 1) == 0, 0, count - 1)).astype(F32)
    area = ya.shape[1]
    widen = ((iota((count, area), 1) >> 5) == iota((count, area), 0)).astype(F32)
    mass = exact(exact(ends, st[4].T), widen)
    stiff = exact(exact(ends, st[1].T), widen)
    upper = iota((SUB, area), 0) < SUB // 2
    ya[...] = jnp.where(upper, stiff, mass)
    yb[...] = jnp.where(upper, mass, 0.0)


def through_z(u, rows_of, mz):
    nt = u(rows_of[0]).shape[1] // LANES
    blocks = [u(i) for i in rows_of]
    tiles = jnp.concatenate([block[:, LANES * t:LANES * (t + 1)] for block in blocks for t in range(nt)], axis=0)
    tiles = swap(tiles.reshape(-1, SUB, LANES)).reshape(-1, LANES)
    hi, lo = split(tiles)
    return mul(jnp.concatenate([hi, lo, hi], axis=1), mz)


def through_y(z, my, ym):
    rows = ym.shape[0]
    packed = []
    for slot in range(2):
        part = z[:, slot * LANES:(slot + 1) * LANES]
        wide = jnp.concatenate([part[at:at + rows] for at in range(0, part.shape[0], rows)], axis=1)
        hi, lo = split(wide)
        packed.append(jnp.concatenate([hi, hi, lo], axis=0))
    second = mul(ym, packed[1])
    both = mul(my, packed[0])
    pairs = []
    for at in range(0, rows, 2 * SUB):
        pairs.append((both[2 * at:2 * at + 2 * SUB], both[2 * at + 2 * SUB:2 * at + 4 * SUB] + second[at:at + 2 * SUB]))
    return pairs


def swap_back(terms, n):
    width = terms[0].shape[1] // LANES
    stacked = jnp.stack([term[SUB * n:SUB * (n + 1), LANES * i:LANES * (i + 1)] for term in terms for i in range(width)])
    stacked = swap(stacked)
    return [[stacked[k * width + i] for i in range(width)] for k in range(2)]


def kernel(sizes, start_in, st_in, basis, coef, mx, my, ym, mz, mzt, ya, yb, wt, field,
           zs, zr, xs, xz, xr, ys, yz, yr, es, ez, er, edge_slots, rows, hsend, hrecv, rsend, rrecv, ready, ws, start, st, loads, mid, us):
    nx, ny, nz = sizes
    total = nx * ny * nz
    count, area = start.shape
    nt = area // LANES
    ni = count // SUB
    last = count - 1
    px, py, pz = lax.axis_index("gx"), lax.axis_index("gy"), lax.axis_index("gz")
    me = (px * ny + py) * nz + pz
    coords = (px, py, pz)
    there = [[coords[d] > 0, coords[d] < sizes[d] - 1] for d in range(3)]

    load_start = pltpu.make_async_copy(start_in, start, loads.at[0])
    load_st = pltpu.make_async_copy(st_in, st, loads.at[1])
    load_start.start()
    load_st.start()
    barrier = pltpu.get_barrier_semaphore()

    def peer(k):
        p = lax.rem(me + k, total)
        return (p // (ny * nz), (p // nz) % ny, p % nz)

    def every_peer(act):
        if total > 64:
            def step(k, carry):
                act(peer(k))
                return carry

            lax.fori_loop(1, total, step, 0)
            return
        step = lambda d, k: coords[d] ^ k if sizes[d] & (sizes[d] - 1) == 0 else lax.rem(coords[d] + k, sizes[d])
        around = [[step(d, k) if k else coords[d] for k in range(sizes[d])] for d in range(3)]
        for ky in range(ny - 1, -1, -1):
            for kx in range(nx - 1, -1, -1):
                for kz in range(nz):
                    if kx or ky or kz:
                        act((around[0][kx], around[1][ky], around[2][kz]))

    def neighbours(act):
        around = [(dx, dy, dz) for dx in (-1, 0, 1) for dy in (-1, 0, 1) for dz in (0, -1, 1) if dx or dy or dz]
        for dx, dy, dz in sorted(around, key=lambda step: -2 * abs(step[0]) - abs(step[1])):
            target = (px + dx, py + dy, pz + dz)
            inside = None
            for d, step in enumerate((dx, dy, dz)):
                if step:
                    side = there[d][(step + 1) // 2]
                    inside = side if inside is None else inside & side

            @pl.when(inside)
            def _():
                act(target)

    beside = [(coords[d] > 0).astype(jnp.int32) + (coords[d] < sizes[d] - 1).astype(jnp.int32) for d in range(3)]
    around_me = (1 + beside[0]) * (1 + beside[1]) * (1 + beside[2]) - 1
    amounts = {
        "e": lambda x, y, z: x * y * (1 + z),
        "x": lambda x, y, z: x * (1 + z),
        "y": lambda x, y, z: y * (1 + z),
        "z": lambda x, y, z: z,
    }
    sides = [(0,) if size == 1 else (1,) if size == 2 else (1, 2) for size in sizes]
    slots = {"e": edge_slots, "x": xr, "y": yr, "z": zr}

    rounds = max(sizes) - 2

    def call(r):
        neighbours(lambda target: pl.semaphore_signal(ready.at[r], inc=1, device_id=target, device_id_type=MESH))

    neighbours(lambda target: pl.semaphore_signal(barrier, inc=1, device_id=target, device_id_type=MESH))

    def clear(missing, refs):
        @pl.when(missing)
        def _():
            for ref in refs:
                ref[...] = jnp.zeros_like(ref)

    phases = range(ITERS + 1)
    for phase in phases:
        er[phase, :, SUB // 2:, :] = jnp.zeros((3, SUB // 2, LANES), F32)
    for d in range(2):
        clear(~there[2][d], [zr.at[2 * phase + d] for phase in phases])
        clear(~there[0][d], [xr.at[pl.ds(6 * phase + 3 * d, 3)] for phase in phases])
        clear(~there[1][d], [yr.at[pl.ds(6 * phase + 3 * d, 3)] for phase in phases])
        for z in range(2):
            clear(there[0][d] & ~there[2][z], [xr.at[6 * phase + 3 * d + 1 + z] for phase in phases])
            clear(there[1][d] & ~there[2][z], [yr.at[6 * phase + 3 * d + 1 + z] for phase in phases])
        for e in range(2):
            q = pl.ds(2 * d + e, 1)
            both = there[0][d] & there[1][e]
            clear(~both, [er.at[phase, :, q] for phase in phases])
            for z in range(2):
                clear(both & ~there[2][z], [er.at[phase, 1 + z, q] for phase in phases])

    def shared(index, d):
        return ((index == 0) & there[d][0]) | ((index == last) & there[d][1])

    lane = iota((count, area), 1)
    ia, ib, ic = iota((count, area), 0), lane >> 5, lane & (count - 1)
    half = lambda index, d: jnp.where(shared(index, d), 0.5, 1.0)
    weight = half(ia, 0) * half(ib, 1) * half(ic, 2)
    wt[...] = weight.astype(F32)
    load_start.wait()
    field[...] = start[...] * wt[...]

    lane_c = iota((count, LANES), 1)
    face_c = (lane_c & (count - 1) == 0) | (lane_c & (count - 1) == last)
    even = (lane_c & 1) == 0
    lane8 = iota((SUB, LANES), 1)
    low8, high8 = lane8 < count, lane8 >= LANES - count
    lane1 = iota((1, LANES), 1)
    diag = iota((SUB, LANES), 0) == lane8

    def tile(t):
        return slice(t * LANES, (t + 1) * LANES)

    def halo_copies(phase):
        out = {name: [] for name in ("e", "ez", "x", "xz", "y", "yz", "z")}

        def add(name, src, into, *direction):
            there_all, target = None, {}
            for d, step in enumerate(direction):
                if step is not None:
                    there_all = there[d][step] if there_all is None else there_all & there[d][step]
            target = tuple(c if step is None else c + 2 * step - 1 for c, step in zip(coords, direction))
            copy = pltpu.make_async_remote_copy(
                src_ref=src, dst_ref=into, send_sem=hsend.at[KINDS.index(name[0])],
                recv_sem=hrecv.at[phase % 2, KINDS.index(name[0])], device_id=target, device_id_type=MESH)
            out[name].append((copy, there_all))

        for z in (None, 1, 0):
            back, kind = (0, "") if z is None else (2 - z, "z")
            for d in range(2):
                for e in range(2):
                    q = pl.ds(2 * d + e, 1)
                    src = es.at[phase, q] if z is None else ez.at[phase, z, q]
                    add("e" + kind, src, er.at[phase, back, pl.ds(2 * (1 - d) + 1 - e, 1)], d, e, z)
            for d in range(2):
                src = xs.at[phase, d] if z is None else xz.at[phase, z, d]
                add("x" + kind, src, xr.at[6 * phase + (1 - d) * 3 + back], d, None, z)
            for d in range(2):
                src = ys.at[phase, d] if z is None else yz.at[phase, z, d]
                add("y" + kind, src, yr.at[6 * phase + (1 - d) * 3 + back], None, d, z)
        for d in range(2):
            add("z", zs.at[phase], zr.at[2 * phase + 1 - d], None, None, d)
        return out

    def start_all(copies):
        for copy, exists, *_ in copies:
            @pl.when(exists)
            def _():
                copy.start()

    def across(value, z):
        c = iota(value.shape, 1) & (count - 1)
        if z == 1:
            return jnp.where(c == 0, pltpu.roll(value, LANES - last, 1), 0.0)
        return jnp.where(c == last, pltpu.roll(value, last, 1), 0.0)

    def send_halo(phase):
        copies = halo_copies(phase)

        def send(local, first):
            for t, value in local.items():
                field[:, tile(t)] = value
            for d in range(2):
                row = 0 if d == 0 else last
                for t, value in local.items():
                    xs[phase, d, t:t + 1, :] = value[row:row + 1]
                if first:
                    for e in range(2):
                        es[phase, 2 * d + e:2 * d + e + 1, :] = local[0 if e == 0 else nt - 1][row:row + 1]
            if first:
                for d in range(2):
                    packed = None
                    for i in range(ni):
                        block = local[0 if d == 0 else nt - 1][SUB * i:SUB * (i + 1)]
                        part = jnp.where(low8 if d == 0 else high8, block, 0.0)
                        shift = (count * i + d * count) % LANES
                        part = part if shift == 0 else pltpu.roll(part, shift, 1)
                        packed = part if packed is None else packed + part
                    ys[phase, d] = packed

        def rest():
            start_all(copies["x"])
            start_all(copies["e"])
            start_all(copies["y"])
            for z in range(2):
                ez[phase, z] = across(es[phase], z)
            start_all(copies["ez"])
            for z in range(2):
                for d in range(2):
                    xz[phase, z, d] = across(xs[phase, d], z)
            start_all(copies["xz"])
            for z in range(2):
                for d in range(2):
                    yz[phase, z, d] = across(ys[phase, d], z)
            start_all(copies["yz"])
            packed = None
            for t in range(nt):
                part = jnp.where(face_c, field[:, tile(t)], 0.0)
                part = part if t == 0 else pltpu.roll(part, 2 * t, 1)
                packed = part if packed is None else packed + part
            zs[phase] = packed
            start_all(copies["z"])

        return send, rest

    def take(kind, sem, phases):
        mine = amounts[kind](*beside)
        for amount in sorted({amounts[kind](x, y, z) for x in sides[0] for y in sides[1] for z in sides[2]}):
            if amount:
                @pl.when(mine == amount)
                def _():
                    into = slots[kind].at[pl.ds(0, amount * phases)]
                    pltpu.make_async_copy(into, into, sem).wait()

    def arrive(phase, kind):
        take(kind, hrecv.at[phase % 2, KINDS.index(kind)], 1)

    def sent(kind):
        take(kind, hsend.at[KINDS.index(kind)], ITERS + 1)

    def add_yz(phase):
        arrive(phase, "z")
        merged = jnp.where(even, pltpu.roll(zr[2 * phase], LANES - last, 1), pltpu.roll(zr[2 * phase + 1], last, 1))
        for t in range(nt):
            part = merged if t == 0 else pltpu.roll(merged, LANES - 2 * t, 1)
            field[:, tile(t)] += jnp.where(face_c, part, 0.0)
        arrive(phase, "y")
        for d in range(2):
            received = yr[6 * phase + 3 * d] + yr[6 * phase + 3 * d + 1] + yr[6 * phase + 3 * d + 2]
            for i in range(ni):
                shift = (-count * i - d * count) % LANES
                part = received if shift == 0 else pltpu.roll(received, shift, 1)
                field[SUB * i:SUB * (i + 1), tile(0 if d == 0 else nt - 1)] += jnp.where(low8 if d == 0 else high8, part, 0.0)

    def add_x(phase):
        arrive(phase, "x")
        for d in range(2):
            row = 0 if d == 0 else last
            received = xr[6 * phase + 3 * d] + xr[6 * phase + 3 * d + 1] + xr[6 * phase + 3 * d + 2]
            for t in range(nt):
                field[row:row + 1, tile(t)] += received[t:t + 1]

    def take_edges(phase, factor):
        arrive(phase, "e")
        out = er[phase, 0] + er[phase, 1] + er[phase, 2]
        side = (iota((SUB, LANES), 0) & 1) == 0
        out = jnp.where((side & high8) | (~side & low8), out, 0.0)
        return out if factor is None else out * factor

    def lines_of(edges):
        twice = edges + pltpu.roll(edges, SUB // 2, 0)
        twice = jnp.concatenate([twice, jnp.zeros_like(twice)], axis=0)
        hi, lo = split(twice)
        z = mul(jnp.concatenate([hi, lo, hi], axis=1), mzt[...])[:SUB]
        out = []
        for t in range(nt):
            line = ya[:, tile(t)] * z[:, :LANES] + yb[:, tile(t)] * z[:, LANES:]
            hi = line.astype(BF16).astype(F32)
            out.append(jnp.concatenate([hi, hi, line - hi, jnp.zeros_like(hi)], axis=0).astype(BF16))
        return out

    def add_edges(k, edges):
        for d in range(2):
            row = 0 if d == 0 else last
            ws[k, row:row + 1, tile(0)] += pltpu.roll(edges[2 * d:2 * d + 1], count, 1)
            ws[k, row:row + 1, tile(nt - 1)] += pltpu.roll(edges[2 * d + 1:2 * d + 2], LANES - count, 1)

    def send_dots(phase, products):
        line = None
        for base in range(0, len(products), SUB):
            packed = None
            for k, product in enumerate(products[base:base + SUB]):
                acc = None
                for i in range(ni):
                    for t in range(nt):
                        block = product[SUB * i:SUB * (i + 1), tile(t)]
                        acc = block if acc is None else acc + block
                part = jnp.where(iota((SUB, LANES), 0) == k, jnp.sum(acc, axis=0, keepdims=True), 0.0)
                packed = part if packed is None else packed + part
            sums = jnp.sum(packed, axis=1, keepdims=True)
            part = jnp.sum(jnp.where(lane8 == iota((SUB, LANES), 0) + base, sums, 0.0), axis=0, keepdims=True)
            line = part if line is None else line + part
        rows[phase, me] = line

        def send(target):
            pltpu.make_async_remote_copy(
                src_ref=rows.at[phase, me], dst_ref=rows.at[phase, me], send_sem=rsend.at[phase],
                recv_sem=rrecv.at[phase], device_id=target, device_id_type=MESH).start()

        every_peer(send)

    def take_dots(phase, amount):
        others = rows.at[phase, pl.ds(0, total - 1)]
        pltpu.make_async_copy(others, others, rrecv.at[phase]).wait()
        line = jnp.sum(rows[phase], axis=0)
        out = []
        for base in range(0, amount, SUB):
            sums = jnp.sum(jnp.where(lane8 == iota((SUB, LANES), 0) + base, line, 0.0), axis=1, keepdims=True)
            out += [sums[i:i + 1] for i in range(min(SUB, amount - base))]
        return out

    pl.semaphore_wait(barrier, around_me)
    send, rest = send_halo(0)
    value = field[...]
    send({t: value[:, tile(t)] for t in range(nt)}, True)
    rest()
    load_st.wait()
    build_matrices(st, mx, my, ym, mz, mzt, ya, yb)
    for r in range(rounds):
        call(r)
        if r < rounds - 1:
            pl.semaphore_wait(ready.at[r], around_me)
    gram, rho = {}, []

    def row_of(k):
        weighted = wt[...] * us[k]
        return [weighted * us[i] for i in range(k + 1)]

    def keep(k, sums):
        for i in range(k + 1):
            gram[i, k] = sums[i]

    def gather(k):
        lead = 2 if k < ITERS - 1 else 0
        sums = take_dots(k, lead + k)
        if lead:
            rho.append(sums[1] / sums[0])
        if k > 0:
            keep(k - 1, sums[lead:])

    factor = None

    def advance(k, inner):
        for i in range(ni):
            if (0 < i < ni - 1) == inner:
                part = slice(SUB * i, SUB * (i + 1))
                ws[k, part] = field[part] if k < 2 else field[part] * factor - ws[k - 1, part]

    middle, ends = list(range(1, ni - 1)), [0, ni - 1]
    block = lambda k: lambda i: ws[k, SUB * i:SUB * (i + 1)]
    for k in range(ITERS):
        add_yz(k)
        advance(k, True)
        inner = through_z(block(k), middle, mz[...])
        add_x(k)
        advance(k, False)
        outer = through_z(block(k), ends, mz[...])
        inner = through_y(inner, my[...], ym[...])
        edges = take_edges(k, factor)
        for p in range(nt // 2):
            swapped = [swap_back(inner[p], n) for n in range(2)]
            for j in range(2):
                hi, lo = split(jnp.concatenate([jnp.concatenate(part[j], axis=0) for part in swapped], axis=1))
                mid[p, 2 * j] = hi
                mid[p, 2 * j + 1] = lo
        outer = through_y(outer, my[...], ym[...])
        lines = lines_of(edges)
        send, rest = send_halo(k + 1)
        order = [0, nt - 1] + list(range(1, nt - 1))
        for p in range(nt // 2):
            pair = order[2 * p:2 * p + 2]
            stack = []
            for j in range(2):
                stack += [mid[p, 2 * j], mid[p, 2 * j], mid[p, 2 * j + 1]]
            swapped = [swap_back(outer[p], n) for n in range(2)]
            for j in range(2):
                hi, lo = split(jnp.concatenate([jnp.concatenate(part[j], axis=0) for part in swapped], axis=1))
                stack += [hi, hi, lo]
            stack.append(jnp.concatenate([lines[t] for t in pair], axis=1))
            out = mul(mx[...], jnp.concatenate(stack, axis=0))
            send({t: out[:, LANES * n:LANES * (n + 1)] for n, t in enumerate(pair)}, p == 0)
        rest()
        if k == 0 and rounds > 0:
            pl.semaphore_wait(ready.at[rounds - 1], around_me)
        add_edges(k, edges)
        vector = ws[k]
        products = [wt[...] * vector * vector, field[...] * vector] if k < ITERS - 1 else []
        send_dots(k, products + (row_of(k - 1) if k > 0 else []))
        if k == 0:
            us[0] = vector
        else:
            gather(k - 1)
            factor = 1.0 / rho[k - 1]
            us[k] = vector * factor - us[k - 1]
    add_yz(ITERS)
    advance(ITERS, True)
    add_x(ITERS)
    advance(ITERS, False)
    add_edges(ITERS, take_edges(ITERS, factor))
    us[ITERS] = ws[ITERS] * factor - us[ITERS - 1]
    send_dots(ITERS, row_of(ITERS - 1) + row_of(ITERS))
    gather(ITERS - 1)

    upper, inverse, scale = {}, {}, []

    def column(k):
        for i in range(k):
            total_i = None
            for m in range(i + 1):
                term = inverse[m, i] * gram[m, k]
                total_i = term if total_i is None else total_i + term
            upper[i, k] = total_i
        rest = gram[k, k]
        for i in range(k):
            rest = rest - upper[i, k] * upper[i, k]
        upper[k, k] = jnp.sqrt(rest)
        inverse[k, k] = 1.0 / upper[k, k]
        for i in range(k):
            total_i = None
            for m in range(i, k):
                term = inverse[i, m] * upper[m, k]
                total_i = term if total_i is None else total_i + term
            inverse[i, k] = -total_i * inverse[k, k]
        if k > 0:
            out = us[0] * inverse[0, k]
            for i in range(1, k + 1):
                out = out + us[i] * inverse[i, k]
            basis[k - 1] = out

    for k in range(ITERS - 1):
        column(k)
    for kind in KINDS:
        sent(kind)
    for phase in range(ITERS):
        others = rows.at[phase, pl.ds(0, total - 1)]
        pltpu.make_async_copy(others, others, rsend.at[phase]).wait()
    sums = take_dots(ITERS, 2 * ITERS + 1)
    keep(ITERS - 1, sums)
    keep(ITERS, sums[ITERS:])
    column(ITERS - 1)
    column(ITERS)
    row2, col2 = iota(coef.shape[1:], 0), iota(coef.shape[1:], 1)
    coefs = jnp.zeros(coef.shape[1:], F32)
    for k in range(ITERS):
        step = rho[min(k, ITERS - 2)]
        alpha = step + step * (upper[k, k + 1] * inverse[k, k])
        if k > 0:
            alpha = alpha - rho[k - 1] * (upper[k - 1, k] * inverse[k - 1, k - 1])
        beta = step * (upper[k + 1, k + 1] * inverse[k, k])
        coefs = jnp.where((row2 == 0) & (col2 == k), alpha, coefs)
        coefs = jnp.where((row2 == 1) & (col2 == k), beta, coefs)
    coef[0] = coefs

    others = rows.at[ITERS, pl.ds(0, total - 1)]
    pltpu.make_async_copy(others, others, rsend.at[ITERS]).wait()


def store(basis, coef, basis_out, coef_out, sems):
    copies = [pltpu.make_async_copy(basis.at[i], basis_out.at[i], sems.at[i]) for i in range(ITERS)]
    copies.append(pltpu.make_async_copy(coef, coef_out, sems.at[ITERS]))
    for copy in copies:
        copy.start()
    for copy in copies:
        copy.wait()


def shards(sizes, start, stencils):
    probes, count, area = start.shape[3:]
    nt = area // LANES
    total = sizes[0] * sizes[1] * sizes[2]
    halos = ITERS + 1
    vmem = pl.BlockSpec(memory_space=pltpu.VMEM)
    call_shapes = (jax.ShapeDtypeStruct((ITERS, count, area), F32), jax.ShapeDtypeStruct((1, 2, ITERS), F32))
    call = pl.pallas_call(
        functools.partial(kernel, sizes),
        out_shape=call_shapes,
        in_specs=[pl.BlockSpec(memory_space=pltpu.HBM)] * 2,
        out_specs=(vmem, vmem),
        scratch_shapes=[
            pltpu.VMEM((count, 7 * count), BF16),
            pltpu.VMEM((4 * count, 6 * count), BF16),
            pltpu.VMEM((2 * count, 6 * count), BF16),
            pltpu.VMEM((3 * LANES, 2 * LANES), BF16),
            pltpu.VMEM((3 * LANES, 2 * LANES), BF16),
            pltpu.VMEM((SUB, area), F32),
            pltpu.VMEM((SUB, area), F32),
            pltpu.VMEM((count, area), F32),
            pltpu.VMEM((count, area), F32),
            pltpu.VMEM((halos, count, LANES), F32),
            pltpu.VMEM((halos * 2, count, LANES), F32),
            pltpu.VMEM((halos, 2, nt, LANES), F32),
            pltpu.VMEM((halos, 2, 2, nt, LANES), F32),
            pltpu.VMEM((halos * 6, nt, LANES), F32),
            pltpu.VMEM((halos, 2, SUB, LANES), F32),
            pltpu.VMEM((halos, 2, 2, SUB, LANES), F32),
            pltpu.VMEM((halos * 6, SUB, LANES), F32),
            pltpu.VMEM((halos, 4, LANES), F32),
            pltpu.VMEM((halos, 2, 4, LANES), F32),
            pltpu.VMEM((halos, 3, SUB, LANES), F32),
            pltpu.VMEM((halos * 12, 1, LANES), F32),
            pltpu.VMEM((halos, total, 1, LANES), F32),
            pltpu.SemaphoreType.DMA((len(KINDS),)),
            pltpu.SemaphoreType.DMA((2, len(KINDS))),
            pltpu.SemaphoreType.DMA((halos,)),
            pltpu.SemaphoreType.DMA((halos,)),
            pltpu.SemaphoreType.REGULAR((max(1, max(sizes) - 2),)),
            pltpu.VMEM((halos, count, area), F32),
            pltpu.VMEM((count, area), F32),
            pltpu.VMEM(stencils.shape[:1] + stencils.shape[4:], F32),
            pltpu.SemaphoreType.DMA((2,)),
            pltpu.VMEM((nt // 2, 4, 2 * SUB, 2 * LANES), BF16),
            pltpu.VMEM((halos, count, area), F32),
        ],
        compiler_params=pltpu.CompilerParams(collective_id=0, has_side_effects=True, vmem_limit_bytes=48 * 1024 * 1024),
    )
    hbm = pl.BlockSpec(memory_space=pltpu.HBM)
    put = pl.pallas_call(
        store,
        out_shape=call_shapes,
        in_specs=[vmem, vmem],
        out_specs=(hbm, hbm),
        scratch_shapes=[pltpu.SemaphoreType.DMA((ITERS + 1,))],
        compiler_params=pltpu.CompilerParams(vmem_limit_bytes=4 * 1024 * 1024),
    )
    results = [put(*call(*(pltpu.with_memory_space_constraint(x, pltpu.HBM) for x in (start[0, 0, 0, p], stencils[:, 0, 0, 0])))) for p in range(probes)]
    basis = jnp.stack([r[0] for r in results])
    return basis[None, None, None], jnp.concatenate([r[1] for r in results])


def solution(mesh):
    sizes = tuple(mesh.shape[name] for name in ("gx", "gy", "gz"))
    return jax.shard_map(
        functools.partial(shards, sizes),
        mesh=mesh,
        in_specs=(P("gx", "gy", "gz", None, None, None), P(None, "gx", "gy", "gz", None, None)),
        out_specs=(P("gx", "gy", "gz", None, None, None, None), P()),
        check_vma=False,
    )
```
